256 devices in a mesh: groups: 2 (over z), tensor: 128 (over x, y, core).
Axes of the slice: x: 8, y: 8, z: 2, core: 2. Of those that a mesh axis runs over, the one named last changes fastest.
The devices are a block of a 8x8x16 slice.
Arguments:
- image_features: bfloat16 [256, 12800], P('groups', 'tensor'), parts along dimension 0, may hold values from -6 to 6
- image_counts: int32 [4], P('groups'), parts along dimension 0, may hold values from 1 to 64, 80 in all
- slot_position: int32 [256], P('groups'), parts along dimension 0, may hold values from 0 to 255, as said below
- text_ids: int32 [512], P('groups'), parts along dimension 0, may hold values from 0 to 49151
- norm_gain: float32 [12800], replicated, may hold values from 0.5 to 1.5
- norm_bias: float32 [12800], replicated, may hold values from -3 to 3
- proj_first: bfloat16 [6144, 12800], P('tensor'), may hold values from -0.0546875 to 0.0546875
- proj_second: bfloat16 [6144, 6144], P('tensor'), may hold values from -0.078125 to 0.078125
- embedding: bfloat16 [6144, 49152], P('tensor'), may hold values from -6 to 6
- rms_gain: float32 [6144], replicated, may hold values from 0.5 to 1.5
- gate_weight: bfloat16 [6144, 16384], P(None, 'tensor'), may hold values from -0.3125 to 0.3125
- up_weight: bfloat16 [6144, 16384], P(None, 'tensor'), may hold values from -0.3125 to 0.3125
- down_weight: bfloat16 [16384, 6144], P('tensor'), may hold values from -0.046875 to 0.046875
- output_grad: bfloat16 [512, 6144], P('groups', 'tensor'), parts along dimension 0, may hold values from -6 to 6
Outputs:
- input_grad: float32 [512, 6144], P('groups', 'tensor'), parts along dimension 0
- second_grad: float32 [12288, 6144], P(('groups', 'tensor')), parts along dimension 0
The draws below stay inside these ranges and needn't reach their ends.
There are 2 independent parts, one for each index of `groups`. The reference program is written for one: setup_inputs(seed, part) draws one part's arguments, and reference() takes and returns one part's arrays. A program takes and returns all parts, laid end to end along the dimension named above; an argument that names none is the same for every part. Nothing has to cross between parts.
Inputs may be any that keep to these rules, and one draw needn't show every extreme that they name: `image_counts`: the counts sum to 80. `slot_position`: the 128 positions are distinct.
All inputs are finite; a program needn't handle non-finite values.
Results may differ from the reference program's by a relative error of at most 0.0079.
Values may be sent and summed in bfloat16 or wider, within the bound.
A program may use at most 128 MiB of HBM per device.

```python
import math
import jax
import jax.numpy as jnp
import numpy as np
from jax import lax

PIX = 12800
D = 6144
FF = 16384
VOCAB = 49152
CAP = 64
IMAGES = 2
SLOTS = 128
LIVE = 80
SEQ = 256


def draw_slot_position(key, part):
    return jax.random.permutation(jax.random.fold_in(key, 17), SEQ)[:SLOTS].astype(jnp.int32)


def place_ends(array, rng, least, top_value):
    dims = array.shape
    index_at = [jax.random.randint(jax.random.fold_in(rng, axis), (), 0, dims[axis]) for axis in range(len(dims))]
    array = array.at[tuple(index_at)].set(least)
    longest = dims.index(max(dims))
    index_at[longest] = (index_at[longest] + 1) % dims[longest]
    return array.at[tuple(index_at)].set(top_value)


def raised(values, key, source, target, shards_of, factor):
    def block_of(axis_at):
        return (jnp.arange(values.shape[axis_at]) // (values.shape[axis_at] // shards_of)).reshape((-1,) + (1,) * (values.ndim - 1 - axis_at))

    one_side = jax.random.permutation(key, shards_of)[block_of(target)]
    other_side = (block_of(target) + shards_of // 2) % shards_of
    return jnp.where((block_of(source) == one_side) | (block_of(source) == other_side), factor * values, values)


def block_levels(stream_key, shape, cuts, low, largest):
    def one(dim, shards_of):
        draws = jax.random.uniform(jax.random.fold_in(jax.random.fold_in(stream_key, 6), dim), (shards_of,), jnp.float32, low / len(cuts), largest / len(cuts))
        return jnp.repeat(jnp.exp(draws), shape[dim] // shards_of).reshape((-1,) + (1,) * (len(shape) - dim - 1))

    level = one(*cuts[0])
    for cut in cuts[1:]:
        level = level * one(*cut)
    return level


def cumulative_ranks(amount, lean):
    weights = [(1 << 20) // math.isqrt(rank ** lean) + 1 for rank in range(1, amount + 1)]
    scale = 1 + sum(weights) // (1 << 30)
    return np.cumsum(np.array([max(1, weight // scale) for weight in weights]))


def ranked(rng, dims, count, skew):
    table = cumulative_ranks(count, skew)
    lot = jax.random.randint(jax.random.fold_in(rng, 1), dims, 0, int(table[count - 1]))
    rank = jnp.searchsorted(jnp.asarray(table, jnp.int32), lot, side="right")
    return jax.random.permutation(jax.random.fold_in(rng, 2), count)[rank].astype(jnp.int32)


def split_up(number_of, total, most, slope):
    loads = [(1 << 20) // math.isqrt(standing ** slope) + 1 for standing in range(2, number_of + 1)]
    surplus, given = total - most - (number_of - 1), [1] * (number_of - 1)
    while surplus > 0:
        free = [i for i in range(number_of - 1) if given[i] < most]
        whole, left = sum([loads[i] for i in free]), surplus
        for i in free:
            extra = min(most - given[i], max(1, left * loads[i] // whole), surplus)
            given[i] = given[i] + extra
            surplus = surplus - extra
    return np.array([most] + given)


def uneven(stream_key, count, total, limit, lean):
    if count == 2:
        one = jax.random.randint(stream_key, (), max(1, total - limit), min(limit, total - 1) + 1)
        return jnp.stack([one, total - one])
    tallies = jnp.asarray(split_up(count, total, limit, lean), jnp.int32)
    couples = (count - 1) // 2
    giver, sink = tallies[1:1 + 2 * couples:2], tallies[2:2 + 2 * couples:2]
    slack = jnp.minimum(giver - 1, limit - sink)
    passed = jax.random.randint(jax.random.fold_in(stream_key, 1), (couples,), 0, 1 << 20) % (slack + 1)
    tallies = tallies.at[1:1 + 2 * couples:2].set(giver - passed).at[2:2 + 2 * couples:2].set(sink + passed)
    return tallies[jax.random.permutation(jax.random.fold_in(stream_key, 2), count)]


def centred(rng, extent, scale, bound, shards=(), kind=jnp.bfloat16):
    loudness = block_levels(rng, extent, shards, -0.22, 0.18) if shards else 1.0
    entries = jax.random.normal(rng, extent, jnp.float32) * scale * loudness
    return jnp.minimum(jnp.maximum(entries, -bound), bound).astype(kind)


def bell_draw_with(rng, shape, deviation, reach, split, heavy, kind=jnp.bfloat16):
    result = deviation * jax.random.normal(rng, shape, jnp.float32)
    if split:
        result = result * block_levels(rng, shape, split, -0.22, 0.18)
    return jnp.clip(raised(result, jax.random.fold_in(rng, 3), *heavy), -reach, reach).astype(kind)


def setup_inputs(seed: int = 0, part: int = 0) -> dict:
    streams_of = jax.random.split(jax.random.key(seed), 15)
    part_keys = jax.random.split(jax.random.fold_in(streams_of[14], part), 15)
    return {
        "image_features": centred(part_keys[0], (SLOTS, PIX), 1.0, 6.0, ((1, 128),)),
        "image_counts": uneven(part_keys[1], IMAGES, LIVE, CAP, 2).astype(jnp.int32),
        "slot_position": draw_slot_position(jax.random.fold_in(jax.random.fold_in(streams_of[14], part), 71), part),
        "text_ids": place_ends(ranked(part_keys[3], (SEQ,), VOCAB, 2), jax.random.fold_in(part_keys[3], 3), 0, VOCAB - 1).astype(jnp.int32),
        "norm_gain": jnp.clip(1.0 + 0.1 * jax.random.normal(streams_of[4], (PIX,), jnp.float32), 0.5, 1.5),
        "norm_bias": centred(streams_of[5], (PIX,), 0.5, 3.0, (), jnp.float32),
        "proj_first": centred(streams_of[6], (D, PIX), PIX ** -0.5, 0.0546875, ((0, 128),)),
        "proj_second": centred(streams_of[7], (D, D), D ** -0.5, 0.078125, ((0, 128),)),
        "embedding": centred(streams_of[8], (D, VOCAB), 1.0, 6.0, ((0, 128),)),
        "rms_gain": jnp.clip(1.0 + 0.1 * jax.random.normal(streams_of[9], (D,), jnp.float32), 0.5, 1.5),
        "gate_weight": bell_draw_with(streams_of[10], (D, FF), D ** -0.5, 0.3125, ((1, 128),), (1, 0, 128, 5.5)),
        "up_weight": bell_draw_with(streams_of[11], (D, FF), D ** -0.5, 0.3125, ((1, 128),), (1, 0, 128, 5.5)),
        "down_weight": centred(streams_of[12], (FF, D), FF ** -0.5, 0.046875, ((0, 128),)),
        "output_grad": centred(part_keys[13], (SEQ, D), 1.0, 6.0, ((1, 128),)),
    }


def reference(image_features, image_counts, slot_position, text_ids, norm_gain, norm_bias, proj_first, proj_second, embedding, rms_gain, gate_weight, up_weight, down_weight, output_grad):
    slot_ids = jnp.arange(SLOTS, dtype=jnp.int32)
    is_live = slot_ids % CAP < jnp.repeat(image_counts, CAP, total_repeat_length=SLOTS)
    values = image_features.astype(jnp.float32)
    centre = values - lax.optimization_barrier(jnp.mean(values, axis=-1, keepdims=True))
    spread = lax.optimization_barrier(jnp.mean(centre * centre, axis=-1, keepdims=True))
    normed = (centre * lax.rsqrt(spread + 1e-05) * norm_gain + norm_bias).astype(jnp.bfloat16)
    hidden_pre = lax.dot_general(normed, proj_first, (((1,), (1,)), ((), ())), preferred_element_type=jnp.float32)
    hidden_act = jax.nn.gelu(hidden_pre, approximate=False).astype(jnp.bfloat16)
    projected = lax.dot_general(hidden_act, proj_second, (((1,), (1,)), ((), ())), preferred_element_type=jnp.float32).astype(jnp.bfloat16)
    target = jnp.where(is_live, slot_position, SEQ).astype(jnp.int32)
    text_rows = jnp.take(embedding, text_ids, axis=1).T
    tokens = text_rows.at[target].set(projected, mode='drop')
    token_values = tokens.astype(jnp.float32)
    inverse = lax.rsqrt(lax.optimization_barrier(jnp.mean(token_values * token_values, axis=-1, keepdims=True)) + 1e-05)
    unit = token_values * inverse
    normed_tokens = (unit * rms_gain).astype(jnp.bfloat16)
    gate_out = jnp.dot(normed_tokens, gate_weight, preferred_element_type=jnp.float32)
    up_out = jnp.dot(normed_tokens, up_weight, preferred_element_type=jnp.float32)
    hidden_grad = lax.dot_general(output_grad, down_weight, (((1,), (1,)), ((), ())), preferred_element_type=jnp.float32)
    sig_gate = jax.nn.sigmoid(gate_out)
    gate_grad = (hidden_grad * up_out * sig_gate * (1.0 + gate_out * (1.0 - sig_gate))).astype(jnp.bfloat16)
    up_grad = (hidden_grad * gate_out * sig_gate).astype(jnp.bfloat16)
    norm_grad = lax.dot_general(gate_grad, gate_weight, (((1,), (1,)), ((), ())), preferred_element_type=jnp.float32)
    norm_grad = norm_grad + lax.dot_general(up_grad, up_weight, (((1,), (1,)), ((), ())), preferred_element_type=jnp.float32)
    scaled = rms_gain * norm_grad
    row_dots = lax.optimization_barrier(jnp.sum(scaled * unit, axis=-1, keepdims=True))
    input_grad = output_grad.astype(jnp.float32) + inverse * (scaled - unit * row_dots / D)
    proj_grad = jnp.where(is_live[:, None], input_grad[slot_position], 0.0).astype(jnp.bfloat16)
    second_grad = lax.dot_general(proj_grad, hidden_act, (((0,), (0,)), ((), ())), preferred_element_type=jnp.float32)
    return (input_grad, second_grad)
```

```python
import jax
import jax.numpy as jnp
from jax import lax
from jax.experimental import pallas as pl
from jax.experimental.pallas import tpu as pltpu
from jax.sharding import Mesh
from jax.sharding import PartitionSpec as P

LIVE = 80
TENSOR = ("tensor_0", "tensor_1", "tensor_2")
GROUPS_TENSOR = ("groups", "tensor_0", "tensor_1", "tensor_2")
MESH = pl.DeviceIdType.MESH
F32 = jnp.float32
BF16 = jnp.bfloat16
NT = (((1,), (1,)), ((), ()))
NN = (((1,), (0,)), ((), ()))
LANES = 128


def dot(a, b, dims=NN):
    return lax.dot_general(a, b, dims, preferred_element_type=F32)


def erf(x):
    x = jnp.clip(x, -3.832506856900711, 3.832506856900711)
    s = x * x
    top = jnp.full_like(x, 0.00022905065861350646)
    for k in (
        0.0034082910107109506,
        0.050955695062380861,
        0.18520832239976145,
        1.128379143519084,
    ):
        top = top * s + k
    low = jnp.full_like(x, -1.1791602954361697e-7)
    for k in (
        0.000023547966471313185,
        0.0010179625278914885,
        0.014070470171167667,
        0.11098505178285362,
        0.49746925110067538,
        1.0,
    ):
        low = low * s + k
    return x * top / low


class Torus:
    def __init__(self):
        self.c = lax.axis_index("tensor_2")
        self.x = lax.axis_index("tensor_0")
        self.y = lax.axis_index("tensor_1")
        self.n = lax.axis_size("tensor_0")
        self.p = self.pick(self.x, self.y)
        self.q = self.pick(self.y, self.x)
        self.me = self.block(self.p, self.q)
        self.partner = {"tensor_0": self.x, "tensor_1": self.y, "tensor_2": 1 - self.c}

    def pick(self, a, b):
        return (1 - self.c) * a + self.c * b

    def dev(self, p, q):
        return {"tensor_0": self.pick(p, q), "tensor_1": self.pick(q, p), "tensor_2": self.c}

    def chip(self, p, q):
        return self.pick(p, q) * self.n + self.pick(q, p)

    def block(self, p, q):
        return self.chip(p, q) * 2 + self.c

    def turn(self, a, d):
        return lax.rem(a + d + self.n, self.n)


class Gather:
    def __init__(self, t, buf, near, plus, minus, mate, sent):
        self.t, self.buf = t, buf
        self.near, self.plus, self.minus, self.mate, self.sent = near, plus, minus, mate, sent

    def copy(self, j, dev, sem):
        return pltpu.make_async_remote_copy(
            self.buf.at[j], self.buf.at[j], self.sent, sem, device_id=dev, device_id_type=MESH
        )

    def to_mate(self, j):
        self.copy(j, self.t.partner, self.mate.at[0]).start()

    def got(self, j, sem):
        self.copy(j, self.t.partner, sem).wait_recv()

    def start(self):
        t = self.t

        @pl.loop(1, t.n)
        def _(d):
            self.copy(t.me, t.dev(t.turn(t.p, d), t.q), self.near.at[d]).start()

        self.to_mate(t.me)

    def ring(self, j, d, hop, up, down):
        t = self.t
        if up:
            self.copy(j, t.dev(t.p, t.turn(t.q, 1)), self.plus.at[hop, d]).start()
        if down:
            self.copy(j, t.dev(t.p, t.turn(t.q, -1)), self.minus.at[hop, d]).start()

    def hop0(self):
        t = self.t
        self.ring(t.me, 0, 0, True, True)

        @pl.loop(1, t.n)
        def _(d):
            j = t.block(t.turn(t.p, -d), t.q)
            self.got(j, self.near.at[d])
            self.ring(j, d, 0, True, True)
            self.to_mate(j)

    def hop(self, h):
        t = self.t
        half = t.n // 2

        def up(d, on):
            j = t.block(t.turn(t.p, -d), t.turn(t.q, -h))
            self.got(j, self.plus.at[h - 1, d])
            self.ring(j, d, h, on, False)
            self.to_mate(j)

        def down(d, on):
            j = t.block(t.turn(t.p, -d), t.turn(t.q, h))
            self.got(j, self.minus.at[h - 1, d])
            self.ring(j, d, h, False, on)
            self.to_mate(j)

        if h < half - 1:

            @pl.loop(0, t.n)
            def _(d):
                up(d, True)
                down(d, True)

        elif h == half - 1:

            @pl.loop(0, half)
            def _(d):
                up(d, True)
                down(d + half, True)
                down(d, False)
                up(d + half, False)

        else:

            @pl.loop(0, half)
            def _(d):
                up(d, False)
                down(d + half, False)

    def finish(self):
        half = self.buf.at[pl.ds(0, self.buf.shape[0] // 2)]
        pltpu.make_async_remote_copy(
            half, half, self.sent, self.mate.at[0], device_id=self.t.partner, device_id_type=MESH
        ).wait_recv()

    def drain(self):
        most = self.buf.at[pl.ds(0, self.buf.shape[0] - 1)]
        pltpu.make_async_remote_copy(
            most, most, self.sent, self.mate.at[0], device_id=self.t.partner, device_id_type=MESH
        ).wait_send()


class Scatter:
    def __init__(self, t, part, give, take, out_up, out_dn, in_up, in_dn, fin_out, fin_in, sems):
        self.t, self.part, self.give, self.take = t, part, give, take
        self.out_up, self.out_dn, self.in_up, self.in_dn = out_up, out_dn, in_up, in_dn
        self.fin_out, self.fin_in = fin_out, fin_in
        self.sent, self.mate, self.s_up, self.s_dn, self.s_fin = sems

    def mate_copy(self):
        return pltpu.make_async_remote_copy(
            self.give,
            self.take,
            self.sent.at[0],
            self.mate.at[0],
            device_id=self.t.partner,
            device_id_type=MESH,
        )

    def start(self):
        t = self.t

        @pl.loop(0, self.give.shape[0])
        def _(i):
            self.give[i] = self.part[2 * i + 1 - t.c].astype(BF16)

        self.mate_copy().start()

    def mated(self):
        self.mate_copy().wait_recv()

    def base(self, p, q):
        t = self.t
        i = t.chip(p, q)
        return self.part[2 * i + t.c] + self.take[i].astype(F32)

    def up_copy(self, s, d):
        t = self.t
        return pltpu.make_async_remote_copy(
            self.out_up.at[s, d],
            self.in_up.at[s, d],
            self.sent.at[0],
            self.s_up.at[s, d],
            device_id=t.dev(t.p, t.turn(t.q, 1)),
            device_id_type=MESH,
        )

    def dn_copy(self, s, d):
        t = self.t
        return pltpu.make_async_remote_copy(
            self.out_dn.at[s, d],
            self.in_dn.at[s, d],
            self.sent.at[0],
            self.s_dn.at[s, d],
            device_id=t.dev(t.p, t.turn(t.q, -1)),
            device_id_type=MESH,
        )

    def step(self, s):
        t = self.t
        half = t.n // 2
        far = half - s

        def up(d, had):
            value = self.base(t.turn(t.p, -d), t.turn(t.q, far))
            if had:
                self.up_copy(s - 1, d).wait_recv()
                value = value + self.in_up[s - 1, d].astype(F32)
            self.out_up[s, d] = value.astype(BF16)
            self.up_copy(s, d).start()

        def dn(d, had):
            value = self.base(t.turn(t.p, -d), t.turn(t.q, -far))
            if had:
                self.dn_copy(s - 1, d).wait_recv()
                value = value + self.in_dn[s - 1, d].astype(F32)
            self.out_dn[s, d] = value.astype(BF16)
            self.dn_copy(s, d).start()

        if s == 0:

            @pl.loop(0, half)
            def _(d):
                up(d, False)
                dn(d + half, False)

        elif s == 1:

            @pl.loop(0, half)
            def _(d):
                up(d, True)
                dn(d + half, True)
                up(d + half, False)
                dn(d, False)

        else:

            @pl.loop(0, t.n)
            def _(d):
                up(d, True)
                dn(d, True)

    def fin_copy(self, d):
        t = self.t
        return pltpu.make_async_remote_copy(
            self.fin_out.at[d],
            self.fin_in.at[d],
            self.sent.at[0],
            self.s_fin.at[d],
            device_id=t.dev(t.turn(t.p, -d), t.q),
            device_id_type=MESH,
        )

    def whole(self, d):
        t = self.t
        last = t.n // 2 - 1
        value = self.base(t.turn(t.p, -d), t.q)
        self.up_copy(last, d).wait_recv()
        self.dn_copy(last, d).wait_recv()
        return value + self.in_up[last, d].astype(F32) + self.in_dn[last, d].astype(F32)

    def last(self):
        t = self.t

        @pl.loop(1, t.n)
        def _(d):
            self.fin_out[d] = self.whole(d).astype(BF16)
            self.fin_copy(d).start()

        return self.whole(0)

    def collect(self, value):
        for d in range(1, self.t.n):
            self.fin_copy(d).wait_recv()
            value = value + self.fin_in[d].astype(F32)
        return value

    def drain(self, like):
        most = like.at[pl.ds(0, like.shape[0] - 1)]
        pltpu.make_async_remote_copy(
            most, most, self.sent.at[0], self.mate.at[0], device_id=self.t.partner, device_id_type=MESH
        ).wait_send()


def kernel_body(
    feats_ref,
    counts_ref,
    pos_ref,
    ids_ref,
    ngain_ref,
    nbias_ref,
    first_hbm,
    second_hbm,
    emb_hbm,
    rgain_ref,
    gate_hbm,
    up_hbm,
    down_hbm,
    og_ref,
    igrad_ref,
    sgrad_ref,
    first_v,
    second_v,
    emb_v,
    wcat,
    down_v,
    wt,
    wpad,
    gpad,
    bpad,
    normed,
    feats_all,
    act_all,
    og_all,
    ta_all,
    tb_all,
    text_own,
    part,
    give,
    take,
    out_up,
    out_dn,
    in_up,
    in_dn,
    fin_out,
    fin_in,
    rd_own,
    rd_mate,
    rd_p,
    rd_pin,
    rd_q,
    rd_qin,
    load_sem,
    near_sem,
    plus_sem,
    minus_sem,
    mate_sem,
    sent_sem,
    rs_sent,
    rs_mate,
    rs_up,
    rs_dn,
    rs_fin,
    rd_sent,
    rd_recv_p,
    rd_recv_q,
    rd_recv_m,
):
    t = Torus()
    n = t.n
    blocks = 2 * n * n
    cols, seq = og_ref.shape
    width, slots = feats_ref.shape
    model = blocks * cols
    pix = blocks * width
    text_b = LANES - LIVE

    loads = [
        pltpu.make_async_copy(first_hbm, first_v, load_sem.at[0]),
        pltpu.make_async_copy(gate_hbm, wcat.at[:, pl.ds(0, LANES)], load_sem.at[1]),
        pltpu.make_async_copy(up_hbm, wcat.at[:, pl.ds(LANES, LANES)], load_sem.at[2]),
        pltpu.make_async_copy(second_hbm, second_v, load_sem.at[3]),
        pltpu.make_async_copy(down_hbm, down_v, load_sem.at[4]),
    ]
    loads[0].start()

    @pl.loop(0, emb_v.shape[0])
    def _(k):
        span = pl.ds(pl.multiple_of(k * LANES, LANES), LANES)
        pltpu.make_async_copy(emb_hbm.at[:, span], emb_v.at[k], load_sem.at[5]).start()

    for load in loads[1:]:
        load.start()

    barrier = pltpu.get_barrier_semaphore()

    @pl.loop(1, n)
    def _(d):
        pl.semaphore_signal(
            barrier, inc=1, device_id=t.dev(t.turn(t.p, d), t.q), device_id_type=MESH
        )
        pl.semaphore_signal(
            barrier, inc=1, device_id=t.dev(t.p, t.turn(t.q, d)), device_id_type=MESH
        )

    pl.semaphore_signal(barrier, inc=1, device_id=t.partner, device_id_type=MESH)

    slot = lax.broadcasted_iota(jnp.int32, (LIVE, slots), 1)
    row = lax.broadcasted_iota(jnp.int32, (LIVE, slots), 0)
    images = counts_ref.shape[0]
    per = slots // images
    at = slot % per
    live = jnp.zeros((LIVE, slots), jnp.int32)
    rank = at
    before = 0
    for k in range(images):
        count = counts_ref[k]
        here = (slot // per) == k
        live = jnp.where(here & (at < count), 1, live)
        rank = jnp.where(here, at + before, rank)
        before = before + count
    choose = jnp.where((live == 1) & (rank == row), 1.0, 0.0).astype(BF16)
    feats_own = dot(choose, feats_ref[...], NT)
    feats_all[t.me] = jnp.zeros((LIVE, LANES), BF16)
    feats_all[t.me, :, 0:width] = feats_own.astype(BF16)

    gathers = []
    for k, buf in enumerate((feats_all, og_all, ta_all, act_all, tb_all)):
        gathers.append(
            Gather(
                t,
                buf,
                near_sem.at[k],
                plus_sem.at[k],
                minus_sem.at[k],
                mate_sem.at[k],
                sent_sem.at[k],
            )
        )
    g_feats, g_og, g_ta, g_act, g_tb = gathers

    pl.semaphore_wait(barrier, 2 * (n - 1) + 1)
    g_feats.start()

    pos = pos_ref[...]
    where_row = lax.broadcasted_iota(jnp.int32, (seq, slots), 0)
    hit = jnp.where((where_row == pos) & (live[0:1] == 1), 1.0, 0.0)
    is_img = jnp.sum(hit, axis=1, keepdims=True)
    img_rank = jnp.sum(hit * rank[0:1].astype(F32), axis=1, keepdims=True)
    low = jnp.where(
        lax.broadcasted_iota(jnp.int32, (seq, seq), 1)
        < lax.broadcasted_iota(jnp.int32, (seq, seq), 0),
        1.0,
        0.0,
    ).astype(BF16)
    not_img = jnp.broadcast_to(1.0 - is_img, (seq, LANES)).astype(BF16)
    text_rank = dot(low, not_img)[:, 0:1]
    text_col = jnp.where(text_rank < LANES, text_rank, text_rank + LIVE)
    col_of = jnp.where(is_img > 0.5, LANES + img_rank, text_col)
    perm = jnp.where(
        lax.broadcasted_iota(jnp.int32, (seq, seq), 1).astype(F32) == col_of, 1.0, 0.0
    ).astype(BF16)
    og_packed = dot(og_ref[...], perm).astype(BF16)
    og_all[t.me] = og_packed
    g_og.start()

    loads[0].wait()
    wpad[...] = jnp.zeros(wpad.shape, BF16)
    gpad[...] = jnp.zeros(gpad.shape, F32)
    bpad[...] = jnp.zeros(bpad.shape, F32)
    for j in range(blocks):
        wpad[:, LANES * j : LANES * j + width] = first_v[:, width * j : width * (j + 1)]
        gpad[j : j + 1, 0:width] = ngain_ref[:, width * j : width * (j + 1)]
        bpad[j : j + 1, 0:width] = nbias_ref[:, width * j : width * (j + 1)]

    g_feats.hop0()

    pltpu.make_async_copy(emb_v, emb_v, load_sem.at[5]).wait()
    lane = lax.broadcasted_iota(jnp.int32, (cols, LANES), 1)

    def embed(tile):
        def one(k, acc):
            word = ids_ref[tile * LANES + k]
            inside = lax.rem(word, LANES)
            found = emb_v[lax.div(word, LANES)].astype(F32)
            column = jnp.sum(jnp.where(lane == inside, found, 0.0), axis=1, keepdims=True)
            return jnp.where(lane == k, column, acc)

        text_own[:, pl.ds(tile * LANES, LANES)] = lax.fori_loop(
            0, LANES, one, jnp.zeros((cols, LANES), F32), unroll=8
        ).astype(BF16)

    embed(0)
    g_feats.hop(1)
    embed(1)
    text_packed = dot(text_own[...], perm)
    text_a = text_packed[:, 0:LANES]
    text_b_tile = text_packed[:, LANES : 2 * LANES]
    ta_all[t.me] = text_a.astype(BF16)
    g_feats.hop(2)
    g_ta.start()

    loads[1].wait()
    loads[2].wait()
    big_eye = jnp.where(
        lax.broadcasted_iota(jnp.int32, (seq, seq), 1)
        == lax.broadcasted_iota(jnp.int32, (seq, seq), 0),
        1.0,
        0.0,
    ).astype(BF16)

    def turn_weights(a, b):
        @pl.loop(a, b)
        def _(k):
            at_row = pl.multiple_of(k * seq, seq)
            flipped = dot(big_eye, wcat[pl.ds(at_row, seq), :], NT)
            wt[:, pl.ds(at_row, seq)] = (flipped * rgain_ref[:, pl.ds(at_row, seq)]).astype(BF16)

    pieces = model // seq
    turn_weights(0, pieces // 2)
    g_feats.hop(3)
    g_og.hop0()
    turn_weights(pieces // 2, pieces)
    g_feats.hop(4)
    g_feats.finish()

    def add_up(k, acc):
        return acc + feats_all[k].astype(F32)

    zero = jnp.zeros((LIVE, LANES), F32)
    total = lax.fori_loop(0, blocks, add_up, zero, unroll=8)
    mean = jnp.sum(total, axis=1, keepdims=True) / pix

    def add_squares(k, acc):
        centre = feats_all[k].astype(F32) - mean
        return acc + centre * centre

    squares = lax.fori_loop(0, blocks, add_squares, zero, unroll=8)
    inside = lax.broadcasted_iota(jnp.int32, (LIVE, LANES), 1) < width
    spread = jnp.sum(jnp.where(inside, squares, 0.0), axis=1, keepdims=True) / pix
    scale = lax.rsqrt(spread + 1e-05)

    @pl.loop(0, blocks)
    def _(k):
        centre = feats_all[k].astype(F32) - mean
        value = centre * scale * gpad[pl.ds(k, 1), :] + bpad[pl.ds(k, 1), :]
        normed[:, pl.ds(pl.multiple_of(k * LANES, LANES), LANES)] = value.astype(BF16)

    depth = 8 * LANES

    def first_step(k, acc):
        span = pl.ds(pl.multiple_of(k * depth, depth), depth)
        return acc + dot(wpad[:, span], normed[:, span], NT)

    hidden = lax.fori_loop(
        0, blocks * LANES // depth, first_step, jnp.zeros((cols, LIVE), F32), unroll=2
    )
    hidden = 0.5 * hidden * (1.0 + erf(hidden * 0.7071067811865476))
    act_all[t.me] = jnp.zeros((cols, LANES), BF16)
    act_all[t.me, :, 0:LIVE] = hidden.astype(BF16)
    g_act.start()

    g_og.hop(1)
    g_act.hop0()
    g_og.hop(2)
    g_act.hop(1)
    g_ta.hop0()
    g_act.hop(2)
    g_og.hop(3)
    g_act.hop(3)
    g_act.hop(4)
    g_act.finish()

    loads[3].wait()
    group = blocks // 8
    span_rows = group * cols

    def rows_of(buf, k):
        return buf[pl.ds(k * group, group)].reshape(span_rows, buf.shape[2])

    def second_step(k, acc):
        span = pl.ds(pl.multiple_of(k * span_rows, span_rows), span_rows)
        return acc + dot(second_v[:, span], rows_of(act_all, k))

    projected = lax.fori_loop(0, 8, second_step, jnp.zeros((cols, LANES), F32))
    tb_all[t.me] = jnp.where(lane < LIVE, projected, text_b_tile).astype(BF16)
    g_tb.start()

    g_og.hop(4)
    g_ta.hop(1)
    g_tb.hop0()
    g_ta.hop(2)
    g_tb.hop(1)
    g_ta.hop(3)
    g_tb.hop(2)
    g_ta.hop(4)
    g_tb.hop(3)
    g_og.finish()
    loads[4].wait()

    def down_step(k, acc):
        span = pl.ds(pl.multiple_of(k * span_rows, span_rows), span_rows)
        return acc + dot(down_v[:, span], rows_of(og_all, k))

    hidden_grad = lax.fori_loop(0, 8, down_step, jnp.zeros((LANES, seq), F32))
    g_ta.finish()

    scatters = []
    for k in range(2):
        scatters.append(
            Scatter(
                t,
                part.at[k],
                give.at[k],
                take.at[k],
                out_up.at[k],
                out_dn.at[k],
                in_up.at[k],
                in_dn.at[k],
                fin_out.at[k],
                fin_in.at[k],
                (rs_sent.at[k], rs_mate.at[k], rs_up.at[k], rs_dn.at[k], rs_fin.at[k]),
            )
        )
    s_a, s_b = scatters

    def gated(buf, hid, k_part):
        def step(k, carry):
            acc, sq = carry
            rows = rows_of(buf, k)
            span = pl.ds(pl.multiple_of(k * span_rows, span_rows), span_rows)
            wide = rows.astype(F32)
            sq = sq + jnp.sum(wide * wide, axis=0, keepdims=True)
            return acc + dot(wt[:, span], rows), sq

        acc, sq = lax.fori_loop(
            0, 8, step, (jnp.zeros((2 * LANES, LANES), F32), jnp.zeros((1, LANES), F32))
        )
        inv = lax.rsqrt(sq / model + 1e-05)
        acc = acc * inv
        gate, up = acc[0:LANES], acc[LANES : 2 * LANES]
        sig = 1.0 / (1.0 + jnp.exp(-gate))
        gate_grad = (hid * up * sig * (1.0 + gate * (1.0 - sig))).astype(BF16)
        up_grad = (hid * gate * sig).astype(BF16)
        dots = jnp.sum(
            gate_grad.astype(F32) * gate + up_grad.astype(F32) * up, axis=0, keepdims=True
        )
        both = jnp.concatenate([gate_grad, up_grad], axis=0)

        @pl.loop(0, 8)
        def _(k):
            at_row = pl.multiple_of(k * span_rows, span_rows)
            value = dot(wcat[pl.ds(at_row, span_rows), :], both)
            part[k_part, pl.ds(k * group, group)] = value.reshape(group, cols, LANES)

        return inv, dots

    inv_a, dots_a = gated(ta_all, hidden_grad[:, 0:LANES], 0)
    s_a.start()
    g_tb.hop(4)
    s_a.mated()
    s_a.step(0)
    g_tb.finish()
    s_a.step(1)
    inv_b, dots_b = gated(tb_all, hidden_grad[:, LANES : 2 * LANES], 1)
    s_b.start()

    rd_own[...] = jnp.zeros(rd_own.shape, F32)
    rd_own[0:1] = dots_a
    rd_own[1:2] = dots_b

    def rd_copy(src, dst, sem_at, recv, dev):
        return pltpu.make_async_remote_copy(
            src, dst, rd_sent.at[sem_at], recv, device_id=dev, device_id_type=MESH
        )

    def rd_m():
        return rd_copy(rd_own, rd_mate, 0, rd_recv_m.at[0], t.partner)

    def rd_along_p(d):
        return rd_copy(rd_p, rd_pin.at[d], 1, rd_recv_p.at[d], t.dev(t.turn(t.p, d), t.q))

    def rd_along_q(d):
        return rd_copy(rd_q, rd_qin.at[d], 2, rd_recv_q.at[d], t.dev(t.p, t.turn(t.q, d)))

    rd_m().start()
    s_b.mated()
    s_b.step(0)
    rd_m().wait_recv()
    rd_p[...] = rd_own[...] + rd_mate[...]

    @pl.loop(1, n)
    def _(d):
        rd_along_p(d).start()

    s_a.step(2)
    s_b.step(1)
    rd_sum = rd_p[...]
    for d in range(1, n):
        rd_along_p(d).wait_recv()
        rd_sum = rd_sum + rd_pin[d]
    rd_q[...] = rd_sum

    @pl.loop(1, n)
    def _(d):
        rd_along_q(d).start()

    s_a.step(3)
    s_b.step(2)
    sum_a = s_a.last()
    s_b.step(3)
    rd_all = rd_q[...]
    for d in range(1, n):
        rd_along_q(d).wait_recv()
        rd_all = rd_all + rd_qin[d]
    own = lax.broadcasted_iota(jnp.int32, (cols, model), 1) == (
        lax.broadcasted_iota(jnp.int32, (cols, model), 0) + t.me * cols
    )
    gain_own = jnp.sum(jnp.where(own, rgain_ref[...], 0.0), axis=1, keepdims=True)
    sum_b = s_b.last()
    grad_a = s_a.collect(sum_a)
    grad_b = s_b.collect(sum_b)

    def update(grad, tokens, inv, dots):
        unit = tokens.astype(F32) * inv
        return inv * (gain_own * grad - unit * (dots / model))

    upd_a = update(grad_a, ta_all[t.me], inv_a, rd_all[0:1])
    upd_b = update(grad_b, tb_all[t.me], inv_b, rd_all[1:2])
    grad_img = og_all[t.me, :, LANES : 2 * LANES].astype(F32) + upd_b
    proj_grad = jnp.where(lane < LIVE, grad_img, 0.0).astype(BF16)

    @pl.loop(0, 8)
    def _(k):
        span = pl.ds(pl.multiple_of(k * span_rows, span_rows), span_rows)
        sgrad_ref[:, span] = dot(proj_grad, rows_of(act_all, k), NT)

    upd = jnp.concatenate([upd_a, upd_b], axis=1)
    high = upd.astype(BF16)
    rest = upd - high.astype(F32)
    mid = rest.astype(BF16)
    small = (rest - mid.astype(F32)).astype(BF16)
    moved = dot(high, perm, NT) + (dot(mid, perm, NT) + dot(small, perm, NT))
    igrad_ref[...] = og_ref[...].astype(F32) + moved

    for g in gathers:
        g.drain()
    s_a.drain(act_all)
    s_b.drain(act_all)
    rd_m().wait_send()
    for k in (1, 2):
        most = rd_pin.at[pl.ds(1, n - 1)]
        rd_copy(most, most, k, rd_recv_m.at[0], t.partner).wait_send()


def on_device(
    image_features,
    image_counts,
    slot_position,
    text_ids,
    norm_gain,
    norm_bias,
    proj_first,
    proj_second,
    embedding,
    rms_gain,
    gate_weight,
    up_weight,
    down_weight,
    output_grad,
):
    n = lax.axis_size("tensor_0")
    blocks = 2 * n * n
    seq, cols = output_grad.shape
    model = blocks * cols
    half = n // 2
    vmem = pl.BlockSpec(memory_space=pltpu.VMEM)
    smem = pl.BlockSpec(memory_space=pltpu.SMEM)
    hbm = pl.BlockSpec(memory_space=pl.ANY)
    dma = pltpu.SemaphoreType.DMA
    tile = (cols, LANES)
    hidden = gate_weight.shape[1]
    igrad, sgrad = pl.pallas_call(
        kernel_body,
        out_shape=(
            jax.ShapeDtypeStruct((cols, seq), F32),
            jax.ShapeDtypeStruct((cols, model), F32),
        ),
        in_specs=[
            vmem,
            smem,
            vmem,
            smem,
            vmem,
            vmem,
            hbm,
            hbm,
            hbm,
            vmem,
            hbm,
            hbm,
            hbm,
            vmem,
        ],
        out_specs=(vmem, vmem),
        scratch_shapes=[
            pltpu.VMEM(proj_first.shape, BF16),
            pltpu.VMEM(proj_second.shape, BF16),
            pltpu.VMEM((embedding.shape[1] // LANES, cols, LANES), BF16),
            pltpu.VMEM((model, 2 * hidden), BF16),
            pltpu.VMEM(down_weight.shape, BF16),
            pltpu.VMEM((2 * hidden, model), BF16),
            pltpu.VMEM((cols, blocks * LANES), BF16),
            pltpu.VMEM((blocks, LANES), F32),
            pltpu.VMEM((blocks, LANES), F32),
            pltpu.VMEM((LIVE, blocks * LANES), BF16),
            pltpu.VMEM((blocks, LIVE, LANES), BF16),
            pltpu.VMEM((blocks, *tile), BF16),
            pltpu.VMEM((blocks, cols, seq), BF16),
            pltpu.VMEM((blocks, *tile), BF16),
            pltpu.VMEM((blocks, *tile), BF16),
            pltpu.VMEM((cols, seq), BF16),
            pltpu.VMEM((2, blocks, *tile), F32),
            pltpu.VMEM((2, blocks // 2, *tile), BF16),
            pltpu.VMEM((2, blocks // 2, *tile), BF16),
            pltpu.VMEM((2, half, n, *tile), BF16),
            pltpu.VMEM((2, half, n, *tile), BF16),
            pltpu.VMEM((2, half, n, *tile), BF16),
            pltpu.VMEM((2, half, n, *tile), BF16),
            pltpu.VMEM((2, n, *tile), BF16),
            pltpu.VMEM((2, n, *tile), BF16),
            pltpu.VMEM((8, LANES), F32),
            pltpu.VMEM((8, LANES), F32),
            pltpu.VMEM((8, LANES), F32),
            pltpu.VMEM((n, 8, LANES), F32),
            pltpu.VMEM((8, LANES), F32),
            pltpu.VMEM((n, 8, LANES), F32),
            dma((6,)),
            dma((5, n)),
            dma((5, half, n)),
            dma((5, half, n)),
            dma((5, 1)),
            dma((5,)),
            dma((2, 1)),
            dma((2, 1)),
            dma((2, half, n)),
            dma((2, half, n)),
            dma((2, n)),
            dma((3,)),
            dma((n,)),
            dma((n,)),
            dma((1,)),
        ],
        compiler_params=pltpu.CompilerParams(
            collective_id=0, has_side_effects=True, vmem_limit_bytes=64 * 1024 * 1024 - 65536
        ),
        name="projector_step",
    )(
        image_features.T,
        image_counts,
        slot_position.reshape(1, -1),
        text_ids,
        norm_gain.reshape(1, -1),
        norm_bias.reshape(1, -1),
        proj_first,
        proj_second,
        embedding,
        rms_gain.reshape(1, -1),
        gate_weight,
        up_weight,
        down_weight,
        output_grad.T,
    )
    return igrad.T, sgrad


def solution(mesh):
    torus = Mesh(
        mesh.devices.reshape(mesh.shape["groups"], 8, 8, 2),
        ("groups", "tensor_0", "tensor_1", "tensor_2"),
    )
    in_specs = (
        P("groups", TENSOR),
        P("groups"),
        P("groups"),
        P("groups"),
        P(),
        P(),
        P(TENSOR, None),
        P(TENSOR, None),
        P(TENSOR, None),
        P(),
        P(None, TENSOR),
        P(None, TENSOR),
        P(TENSOR, None),
        P("groups", TENSOR),
    )
    out_specs = (P("groups", TENSOR), P(GROUPS_TENSOR, None))
    return jax.shard_map(
        on_device, mesh=torus, in_specs=in_specs, out_specs=out_specs, check_vma=False
    )
```

```python
import jax
import jax.numpy as jnp
from jax import lax
from jax.experimental import pallas as pl
from jax.experimental.pallas import tpu as pltpu
from jax.sharding import Mesh
from jax.sharding import PartitionSpec as P

LIVE = 80
TENSOR = ("tensor_0", "tensor_1", "tensor_2")
GROUPS_TENSOR = ("groups", "tensor_0", "tensor_1", "tensor_2")
MESH = pl.DeviceIdType.MESH
F32 = jnp.float32
BF16 = jnp.bfloat16
NT = (((1,), (1,)), ((), ()))
NN = (((1,), (0,)), ((), ()))
LANES = 128


def dot(a, b, dims=NN):
    return lax.dot_general(a, b, dims, preferred_element_type=F32)


def erf(x):
    x = jnp.clip(x, -3.832506856900711, 3.832506856900711)
    s = x * x
    top = jnp.full_like(x, 0.00022905065861350646)
    for k in (
        0.0034082910107109506,
        0.050955695062380861,
        0.18520832239976145,
        1.128379143519084,
    ):
        top = top * s + k
    low = jnp.full_like(x, -1.1791602954361697e-7)
    for k in (
        0.000023547966471313185,
        0.0010179625278914885,
        0.014070470171167667,
        0.11098505178285362,
        0.49746925110067538,
        1.0,
    ):
        low = low * s + k
    return x * top / low


class Torus:
    def __init__(self):
        self.c = lax.axis_index("tensor_2")
        self.x = lax.axis_index("tensor_0")
        self.y = lax.axis_index("tensor_1")
        self.n = lax.axis_size("tensor_0")
        self.p = self.pick(self.x, self.y)
        self.q = self.pick(self.y, self.x)
        self.me = self.block(self.p, self.q)
        self.partner = {"tensor_0": self.x, "tensor_1": self.y, "tensor_2": 1 - self.c}

    def pick(self, a, b):
        return (1 - self.c) * a + self.c * b

    def dev(self, p, q):
        return {"tensor_0": self.pick(p, q), "tensor_1": self.pick(q, p), "tensor_2": self.c}

    def chip(self, p, q):
        return self.pick(p, q) * self.n + self.pick(q, p)

    def block(self, p, q):
        return self.chip(p, q) * 2 + self.c

    def row(self, hop, down):
        last = self.n // 2 - 1
        return 2 * last if hop == last else hop + down * last

    def turn(self, a, d):
        return lax.rem(a + d + self.n, self.n)


class Gather:
    def __init__(self, t, buf, near, ring, mate, sent):
        self.t, self.buf = t, buf
        self.near, self.sems, self.mate, self.sent = near, ring, mate, sent

    def copy(self, j, dev, sem):
        return pltpu.make_async_remote_copy(
            self.buf.at[j], self.buf.at[j], self.sent, sem, device_id=dev, device_id_type=MESH
        )

    def to_mate(self, j):
        self.copy(j, self.t.partner, self.mate.at[0]).start()

    def got(self, j, sem):
        self.copy(j, self.t.partner, sem).wait_recv()

    def start(self):
        t = self.t

        @pl.loop(1, t.n)
        def _(d):
            self.copy(t.me, t.dev(t.turn(t.p, d), t.q), self.near.at[lax.div(d, 2)]).start()

        self.to_mate(t.me)

    def up(self, j, k, hop):
        t = self.t
        self.copy(j, t.dev(t.p, t.turn(t.q, 1)), self.sems.at[t.row(hop, 0), k]).start()

    def down(self, j, k, hop):
        t = self.t
        self.copy(j, t.dev(t.p, t.turn(t.q, -1)), self.sems.at[t.row(hop, 1), k]).start()

    def hop0(self):
        t = self.t

        def own(j, k):
            self.up(j, k, 0)
            self.down(j, k, 0)

        own(t.me, 0)
        j = t.block(t.turn(t.p, -1), t.q)
        self.got(j, self.near.at[0])
        own(j, 0)
        self.to_mate(j)

        @pl.loop(1, t.n // 2)
        def _(k):
            self.got(pl.ds(0, 2), self.near.at[k])
            for e in range(2):
                j = t.block(t.turn(t.p, -2 * k - e), t.q)
                own(j, k)
                self.to_mate(j)

    def hop(self, h):
        t = self.t
        half = t.n // 2
        few = half // 2

        def up(k, on):
            self.got(pl.ds(0, 2), self.sems.at[t.row(h - 1, 0), k])
            for e in range(2):
                j = t.block(t.turn(t.p, -2 * k - e), t.turn(t.q, -h))
                if on:
                    self.up(j, k, h)
                self.to_mate(j)

        def down(k, on):
            self.got(pl.ds(0, 2), self.sems.at[t.row(h - 1, 1), k])
            for e in range(2):
                j = t.block(t.turn(t.p, -2 * k - e), t.turn(t.q, h))
                if on:
                    self.down(j, k, h)
                self.to_mate(j)

        if h < half - 1:

            @pl.loop(0, half)
            def _(k):
                up(k, True)
                down(k, True)

        elif h == half - 1:

            @pl.loop(0, few)
            def _(k):
                up(k, True)
                down(k + few, True)
                down(k, False)
                up(k + few, False)

        else:

            @pl.loop(0, few)
            def _(k):
                up(k, False)
                down(k + few, False)

    def finish(self):
        half = self.buf.at[pl.ds(0, self.buf.shape[0] // 2)]
        pltpu.make_async_remote_copy(
            half, half, self.sent, self.mate.at[0], device_id=self.t.partner, device_id_type=MESH
        ).wait_recv()

    def drain(self):
        most = self.buf.at[pl.ds(0, self.buf.shape[0] - 1)]
        pltpu.make_async_remote_copy(
            most, most, self.sent, self.mate.at[0], device_id=self.t.partner, device_id_type=MESH
        ).wait_send()


class Leap(Gather):
    def send(self, j, k, far, dist, down):
        t = self.t
        by = -far if down else far
        sem = self.sems.at[t.row(dist - 1, down), k]
        self.copy(j, t.dev(t.p, t.turn(t.q, by)), sem).start()

    def hop0(self):
        t = self.t

        def own(j, k):
            for far in (2, 1):
                for down in (0, 1):
                    self.send(j, k, far, far, down)

        own(t.me, 0)
        j = t.block(t.turn(t.p, -1), t.q)
        self.got(j, self.near.at[0])
        own(j, 0)
        self.to_mate(j)

        @pl.loop(1, t.n // 2)
        def _(k):
            self.got(pl.ds(0, 2), self.near.at[k])
            for e in range(2):
                j = t.block(t.turn(t.p, -2 * k - e), t.q)
                own(j, k)
                self.to_mate(j)

    def arrived(self, k, dist, down, onward):
        t = self.t
        self.got(pl.ds(0, 2), self.sems.at[t.row(dist - 1, down), k])
        for e in range(2):
            by = dist if down else -dist
            j = t.block(t.turn(t.p, -2 * k - e), t.turn(t.q, by))
            for far in onward:
                self.send(j, k, far, dist + far, down)
            self.to_mate(j)

    def relay(self):
        few = self.t.n // 4

        @pl.loop(0, few)
        def _(k):
            self.arrived(k, 2, 0, (2, 1))
            self.arrived(k + few, 2, 1, (2, 1))

        @pl.loop(0, few)
        def _(k):
            self.arrived(k + few, 2, 0, (1,))
            self.arrived(k, 2, 1, (1,))

    def tail(self, dist):
        @pl.loop(0, self.t.n // 2)
        def _(k):
            self.arrived(k, dist, 0, ())
            self.arrived(k, dist, 1, ())

    def tail4(self):
        few = self.t.n // 4

        @pl.loop(0, few)
        def _(k):
            self.arrived(k, 4, 0, ())
            self.arrived(k + few, 4, 1, ())


class Scatter:
    def __init__(self, t, part, give, take, out_up, out_dn, in_up, in_dn, fin_out, fin_in, sems):
        self.t, self.part, self.give, self.take = t, part, give, take
        self.out_up, self.out_dn, self.in_up, self.in_dn = out_up, out_dn, in_up, in_dn
        self.fin_out, self.fin_in = fin_out, fin_in
        self.sent, self.mate, self.ring, self.near = sems

    def mate_copy(self, span):
        return pltpu.make_async_remote_copy(
            self.give.at[span],
            self.take.at[span],
            self.sent.at[0],
            self.mate.at[0],
            device_id=self.t.partner,
            device_id_type=MESH,
        )

    def fill(self, k, even, odd):
        span = pl.ds(k * even.shape[0], even.shape[0])
        self.part[span] = jnp.where(self.t.c == 0, even, odd)
        self.give[span] = jnp.where(self.t.c == 0, odd, even).astype(BF16)
        self.mate_copy(span).start()

    def mated(self):
        self.mate_copy(pl.ds(0, self.give.shape[0])).wait_recv()

    def base(self, p, q):
        t = self.t
        i = t.chip(p, q)
        return self.part[i] + self.take[i].astype(F32)

    def ring_copy(self, dist, d, down):
        t = self.t
        hop = dist if dist < 3 else dist - 2
        out, into = (self.out_dn, self.in_dn) if down else (self.out_up, self.in_up)
        return pltpu.make_async_remote_copy(
            out.at[dist - 1, d],
            into.at[dist - 1, d],
            self.sent.at[0],
            self.ring.at[t.row(dist - 1, down), lax.div(d, 2)],
            device_id=t.dev(t.p, t.turn(t.q, -hop if down else hop)),
            device_id_type=MESH,
        )

    def pair(self, dist, k, down):
        two = (self.in_dn if down else self.in_up).at[dist - 1, pl.ds(2 * k, 2)]
        pltpu.make_async_remote_copy(
            two,
            two,
            self.sent.at[0],
            self.ring.at[self.t.row(dist - 1, down), k],
            device_id=self.t.partner,
            device_id_type=MESH,
        ).wait_recv()

    def send(self, dist, k, down, had):
        t = self.t
        into = self.in_dn if down else self.in_up
        out = self.out_dn if down else self.out_up
        for h in had:
            self.pair(h, k, down)
        for e in range(2):
            d = 2 * k + e
            value = self.base(t.turn(t.p, -d), t.turn(t.q, -dist if down else dist))
            for h in had:
                value = value + into[h - 1, d].astype(F32)
            out[dist - 1, d] = value.astype(BF16)
            self.ring_copy(dist, d, down).start()

    def stage1(self):
        few = self.t.n // 4

        @pl.loop(0, few)
        def _(k):
            self.send(4, k, 0, ())
            self.send(4, k + few, 1, ())

        @pl.loop(0, 2 * few)
        def _(k):
            self.send(3, k, 0, ())
            self.send(3, k, 1, ())

    def stage1b(self):
        @pl.loop(0, self.t.n // 2)
        def _(k):
            self.send(1, k, 0, ())
            self.send(1, k, 1, ())

    def stage2(self):
        few = self.t.n // 4

        @pl.loop(0, few)
        def _(k):
            self.send(2, k, 0, (3, 4))
            self.send(2, k + few, 1, (3, 4))
            self.send(2, k + few, 0, (3,))
            self.send(2, k, 1, (3,))

    def fin_copy(self, d):
        t = self.t
        return pltpu.make_async_remote_copy(
            self.fin_out.at[d],
            self.fin_in.at[d],
            self.sent.at[0],
            self.near.at[lax.div(d, 2)],
            device_id=t.dev(t.turn(t.p, -d), t.q),
            device_id_type=MESH,
        )

    def whole(self, d):
        value = self.base(self.t.turn(self.t.p, -d), self.t.q)
        for into in (self.in_up, self.in_dn):
            for dist in (1, 2):
                value = value + into[dist - 1, d].astype(F32)
        return value

    def last(self):
        t = self.t

        def both(k):
            for down in (0, 1):
                for dist in (1, 2):
                    self.pair(dist, k, down)

        def give(d):
            self.fin_out[d] = self.whole(d).astype(BF16)
            self.fin_copy(d).start()

        both(0)
        give(1)

        @pl.loop(1, t.n // 2)
        def _(k):
            both(k)
            give(2 * k)
            give(2 * k + 1)

        return self.whole(0)

    def collect(self, value):
        self.fin_copy(1).wait_recv()
        value = value + self.fin_in[1].astype(F32)
        for k in range(1, self.t.n // 2):
            two = self.fin_in.at[pl.ds(2 * k, 2)]
            pltpu.make_async_remote_copy(
                two,
                two,
                self.sent.at[0],
                self.near.at[k],
                device_id=self.t.partner,
                device_id_type=MESH,
            ).wait_recv()
            value = value + self.fin_in[2 * k].astype(F32) + self.fin_in[2 * k + 1].astype(F32)
        return value

    def drain(self, like):
        most = like.at[pl.ds(0, like.shape[0] - 1)]
        pltpu.make_async_remote_copy(
            most, most, self.sent.at[0], self.mate.at[0], device_id=self.t.partner, device_id_type=MESH
        ).wait_send()


def kernel_body(
    feats_ref,
    counts_ref,
    pos_ref,
    ids_ref,
    ngain_ref,
    nbias_ref,
    first_hbm,
    second_hbm,
    emb_hbm,
    rgain_ref,
    gate_hbm,
    up_hbm,
    down_hbm,
    og_ref,
    igrad_ref,
    pgrad_ref,
    act_hbm,
    first_v,
    second_v,
    emb_v,
    wcat,
    down_v,
    wt,
    wpad,
    gb_ref,
    feats_all,
    act_all,
    og_all,
    ta_all,
    tb_all,
    text_own,
    part,
    give,
    take,
    out_up,
    out_dn,
    in_up,
    in_dn,
    fin_out,
    fin_in,
    rd_own,
    rd_mate,
    rd_p,
    rd_pin,
    rd_q,
    rd_qin,
    load_sem,
    near_sem,
    ring_sem,
    mate_sem,
    sent_sem,
    rs_sent,
    rs_mate,
    rd_sent,
    rd_recv_p,
    rd_recv_q,
    rd_recv_m,
):
    t = Torus()
    n = t.n
    blocks = 2 * n * n
    cols, seq = og_ref.shape
    width, slots = feats_ref.shape
    model = blocks * cols
    pix = blocks * width

    barrier = pltpu.get_barrier_semaphore()

    @pl.loop(1, n)
    def _(d):
        pl.semaphore_signal(
            barrier, inc=1, device_id=t.dev(t.turn(t.p, d), t.q), device_id_type=MESH
        )
        pl.semaphore_signal(
            barrier, inc=1, device_id=t.dev(t.p, t.turn(t.q, d)), device_id_type=MESH
        )

    pl.semaphore_signal(barrier, inc=1, device_id=t.partner, device_id_type=MESH)

    loads = [
        pltpu.make_async_copy(first_hbm, first_v, load_sem.at[0]),
        pltpu.make_async_copy(gate_hbm, wcat.at[:, pl.ds(0, LANES)], load_sem.at[1]),
        pltpu.make_async_copy(up_hbm, wcat.at[:, pl.ds(LANES, LANES)], load_sem.at[2]),
        pltpu.make_async_copy(second_hbm, second_v, load_sem.at[3]),
        pltpu.make_async_copy(down_hbm, down_v, load_sem.at[4]),
    ]
    loads[0].start()

    slot = lax.broadcasted_iota(jnp.int32, (LIVE, slots), 1)
    row = lax.broadcasted_iota(jnp.int32, (LIVE, slots), 0)
    images = counts_ref.shape[0]
    per = slots // images
    at = slot % per
    live = jnp.zeros((LIVE, slots), jnp.int32)
    rank = at
    before = 0
    for k in range(images):
        count = counts_ref[k]
        here = (slot // per) == k
        live = jnp.where(here & (at < count), 1, live)
        rank = jnp.where(here, at + before, rank)
        before = before + count
    choose = jnp.where((live == 1) & (rank == row), 1.0, 0.0).astype(BF16)
    feats_own = dot(choose, feats_ref[...], NT)
    feats_all[t.me] = jnp.zeros((LIVE, LANES), BF16)
    feats_all[t.me, :, 0:width] = feats_own.astype(BF16)

    gathers = []
    for k, buf in enumerate((feats_all, og_all, ta_all, act_all, tb_all)):
        kind = Leap if k > 2 else Gather
        gathers.append(
            kind(t, buf, near_sem.at[k], ring_sem.at[k], mate_sem.at[k], sent_sem.at[k])
        )
    g_feats, g_og, g_ta, g_act, g_tb = gathers

    pl.semaphore_wait(barrier, 2 * (n - 1) + 1)
    g_feats.start()

    @pl.loop(0, emb_v.shape[0], unroll=8)
    def _(k):
        span = pl.ds(pl.multiple_of(k * LANES, LANES), LANES)
        pltpu.make_async_copy(emb_hbm.at[:, span], emb_v.at[k], load_sem.at[5]).start()

    for load in loads[1:]:
        load.start()

    pos = pos_ref[...]
    where_row = lax.broadcasted_iota(jnp.int32, (seq, slots), 0)
    hit = jnp.where((where_row == pos) & (live[0:1] == 1), 1.0, 0.0)
    is_img = jnp.sum(hit, axis=1, keepdims=True)
    img_rank = jnp.sum(hit * rank[0:1].astype(F32), axis=1, keepdims=True)
    low = jnp.where(
        lax.broadcasted_iota(jnp.int32, (seq, seq), 1)
        < lax.broadcasted_iota(jnp.int32, (seq, seq), 0),
        1.0,
        0.0,
    ).astype(BF16)
    not_img = jnp.broadcast_to(1.0 - is_img, (seq, LANES)).astype(BF16)
    text_rank = dot(low, not_img)[:, 0:1]
    text_col = jnp.where(text_rank < LANES, text_rank, text_rank + LIVE)
    col_of = jnp.where(is_img > 0.5, LANES + img_rank, text_col)
    perm = jnp.where(
        lax.broadcasted_iota(jnp.int32, (seq, seq), 1).astype(F32) == col_of, 1.0, 0.0
    ).astype(BF16)
    og_packed = dot(og_ref[...], perm).astype(BF16)
    og_all[t.me] = og_packed
    g_og.start()

    loads[0].wait()
    wpad[...] = jnp.zeros(wpad.shape, BF16)
    gb_ref[...] = jnp.zeros(gb_ref.shape, F32)
    for j in range(blocks):
        wpad[:, LANES * j : LANES * j + width] = first_v[:, width * j : width * (j + 1)]
        line, start = divmod(width * j, LANES)
        fit = min(width, LANES - start)
        for k, ref in enumerate((ngain_ref, nbias_ref)):
            gb_ref[k, j : j + 1, 0:fit] = ref[line : line + 1, start : start + fit]
            if fit < width:
                gb_ref[k, j : j + 1, fit:width] = ref[line + 1 : line + 2, 0 : width - fit]

    pltpu.make_async_copy(emb_v, emb_v, load_sem.at[5]).wait()
    lane = lax.broadcasted_iota(jnp.int32, (cols, LANES), 1)

    def embed(tile):
        def one(k, acc):
            word = ids_ref[tile * LANES + k]
            inside = lax.rem(word, LANES)
            found = emb_v[lax.div(word, LANES)].astype(F32)
            column = jnp.sum(jnp.where(lane == inside, found, 0.0), axis=1, keepdims=True)
            return jnp.where(lane == k, column, acc)

        text_own[:, pl.ds(tile * LANES, LANES)] = lax.fori_loop(
            0, LANES, one, jnp.zeros((cols, LANES), F32), unroll=8
        ).astype(BF16)

    embed(0)
    embed(1)
    text_packed = dot(text_own[...], perm)
    text_a = text_packed[:, 0:LANES]
    text_b_tile = text_packed[:, LANES : 2 * LANES]
    ta_all[t.me] = text_a.astype(BF16)
    g_ta.start()

    g_feats.hop0()
    g_feats.hop(1)
    g_feats.hop(2)
    g_feats.hop(3)
    g_og.hop0()
    g_feats.hop(4)

    shift = feats_all[t.me].astype(F32)[:, 0:1]

    band = 16
    bands = LIVE // band

    def sums_of(core, carry):
        out = []
        for r in range(bands):
            rows = pl.ds(r * band, band)
            about = jnp.broadcast_to(shift[r * band : (r + 1) * band], (band, LANES))

            def add_up(k, pair):
                moved = feats_all[2 * k + core, rows].astype(F32) - about
                return pair[0] + moved, pair[1] + moved * moved

            out.append(lax.fori_loop(0, blocks // 2, add_up, carry[r], unroll=8))
        return out

    zero = jnp.zeros((band, LANES), F32)
    sums = sums_of(t.c, [(zero, zero)] * bands)
    g_feats.finish()
    sums = sums_of(1 - t.c, sums)
    sums = [jnp.concatenate([sums[r][e] for r in range(bands)], axis=0) for e in range(2)]
    inside = lax.broadcasted_iota(jnp.int32, (LIVE, LANES), 1) < width
    off = jnp.sum(jnp.where(inside, sums[0], 0.0), axis=1, keepdims=True) / pix
    square = jnp.sum(jnp.where(inside, sums[1], 0.0), axis=1, keepdims=True) / pix
    mean = shift + off
    scale = lax.rsqrt(jnp.maximum(square - off * off, 0.0) + 1e-05)
    g_og.hop(1)
    g_ta.hop0()

    fold = 8

    def first_step(k, acc):
        tiles = []
        for e in range(fold):
            j = k * fold + e
            centre = feats_all[j].astype(F32) - mean
            value = centre * scale * gb_ref[0, pl.ds(j, 1), :] + gb_ref[1, pl.ds(j, 1), :]
            tiles.append(value.astype(BF16))
        span = pl.ds(pl.multiple_of(k * fold * LANES, fold * LANES), fold * LANES)
        return acc + dot(wpad[:, span], jnp.concatenate(tiles, axis=1), NT)

    hidden = lax.fori_loop(
        0, blocks // fold, first_step, jnp.zeros((cols, LIVE), F32), unroll=2
    )
    hidden = 0.5 * hidden * (1.0 + erf(hidden * 0.7071067811865476))
    act_all[t.me] = jnp.zeros((cols, LANES), BF16)
    act_all[t.me, :, 0:LIVE] = hidden.astype(BF16)
    g_act.start()

    loads[1].wait()
    loads[2].wait()
    big_eye = jnp.where(
        lax.broadcasted_iota(jnp.int32, (seq, seq), 1)
        == lax.broadcasted_iota(jnp.int32, (seq, seq), 0),
        1.0,
        0.0,
    ).astype(BF16)

    def turn_weights(a, b):
        @pl.loop(a, b, unroll=2)
        def _(k):
            at_row = pl.multiple_of(k * seq, seq)
            flipped = dot(big_eye, wcat[pl.ds(at_row, seq), :], NT)
            wt[:, pl.ds(at_row, seq)] = (flipped * rgain_ref[:, pl.ds(at_row, seq)]).astype(BF16)

    pieces = model // seq
    cut = [pieces * k // 6 for k in range(7)]
    g_og.hop(2)
    turn_weights(cut[0], cut[1])
    g_ta.hop(1)
    turn_weights(cut[1], cut[2])
    g_act.hop0()
    g_og.hop(3)
    turn_weights(cut[2], cut[3])
    g_ta.hop(2)
    turn_weights(cut[3], cut[4])
    g_act.relay()
    g_act.tail(1)
    g_ta.hop(3)
    turn_weights(cut[4], cut[5])
    g_og.hop(4)
    turn_weights(cut[5], cut[6])
    g_act.tail(3)
    g_act.tail4()
    g_act.finish()
    keep = pltpu.make_async_copy(act_all, act_hbm, load_sem.at[6])
    keep.start()

    loads[3].wait()
    group = blocks // 8
    span_rows = group * cols

    def rows_of(buf, k):
        return buf[pl.ds(k * group, group)].reshape(span_rows, buf.shape[2])

    def second_step(k, acc):
        span = pl.ds(pl.multiple_of(k * span_rows, span_rows), span_rows)
        return acc + dot(second_v[:, span], rows_of(act_all, k))

    projected = lax.fori_loop(0, 8, second_step, jnp.zeros((cols, LANES), F32), unroll=8)
    tb_all[t.me] = jnp.where(lane < LIVE, projected, text_b_tile).astype(BF16)
    g_tb.start()

    g_ta.hop(4)
    g_og.finish()
    loads[4].wait()

    def down_step(k, acc):
        span = pl.ds(pl.multiple_of(k * span_rows, span_rows), span_rows)
        return acc + dot(down_v[:, span], rows_of(og_all, k))

    hidden_grad = lax.fori_loop(0, 8, down_step, jnp.zeros((LANES, seq), F32), unroll=4)
    scatters = []
    for k, share in enumerate((0, 3)):
        scatters.append(
            Scatter(
                t,
                part.at[k],
                give.at[k],
                take.at[k],
                out_up.at[k],
                out_dn.at[k],
                in_up.at[k],
                in_dn.at[k],
                fin_out.at[k],
                fin_in.at[k],
                (rs_sent.at[k], rs_mate.at[k], ring_sem.at[share], near_sem.at[share]),
            )
        )
    s_a, s_b = scatters

    def gates(buf, hid):
        def step(k, carry):
            acc, sq = carry
            rows = rows_of(buf, k)
            span = pl.ds(pl.multiple_of(k * span_rows, span_rows), span_rows)
            wide = rows.astype(F32)
            sq = sq + jnp.sum(wide * wide, axis=0, keepdims=True)
            return acc + dot(wt[:, span], rows), sq

        acc, sq = lax.fori_loop(
            0,
            8,
            step,
            (jnp.zeros((2 * LANES, LANES), F32), jnp.zeros((1, LANES), F32)),
            unroll=4,
        )
        inv = lax.rsqrt(sq / model + 1e-05)
        acc = acc * inv
        gate, up = acc[0:LANES], acc[LANES : 2 * LANES]
        sig = 1.0 / (1.0 + jnp.exp(-gate))
        gate_grad = (hid * up * sig * (1.0 + gate * (1.0 - sig))).astype(BF16)
        up_grad = (hid * gate * sig).astype(BF16)
        dots = jnp.sum(
            gate_grad.astype(F32) * gate + up_grad.astype(F32) * up, axis=0, keepdims=True
        )
        both = jnp.concatenate([gate_grad, up_grad], axis=0)

        return inv, dots, both

    def spread_out(both, scatter):
        @pl.loop(0, 8, unroll=2)
        def _(k):
            at_row = pl.multiple_of(k * span_rows, span_rows)
            value = dot(wcat[pl.ds(at_row, span_rows), :], both)
            value = value.reshape(group // 2, 2, cols, LANES)
            scatter.fill(k, value[:, 0], value[:, 1])

    g_ta.finish()
    inv_a, dots_a, both_a = gates(ta_all, hidden_grad[:, 0:LANES])
    g_tb.hop0()
    spread_out(both_a, s_a)
    g_tb.relay()
    s_a.mated()
    s_a.stage1()
    g_tb.tail(1)
    s_a.stage1b()
    g_tb.tail(3)
    g_tb.tail4()
    g_tb.finish()
    inv_b, dots_b, both_b = gates(tb_all, hidden_grad[:, LANES : 2 * LANES])
    s_a.stage2()
    spread_out(both_b, s_b)

    rd_own[...] = jnp.zeros(rd_own.shape, F32)
    rd_own[0:1] = dots_a
    rd_own[1:2] = dots_b

    def rd_copy(src, dst, sem_at, recv, dev):
        return pltpu.make_async_remote_copy(
            src, dst, rd_sent.at[sem_at], recv, device_id=dev, device_id_type=MESH
        )

    def rd_m():
        return rd_copy(rd_own, rd_mate, 0, rd_recv_m.at[0], t.partner)

    def rd_along_p(d):
        return rd_copy(rd_p, rd_pin.at[d], 1, rd_recv_p.at[d], t.dev(t.turn(t.p, d), t.q))

    def rd_along_q(d):
        return rd_copy(rd_q, rd_qin.at[d], 2, rd_recv_q.at[d], t.dev(t.p, t.turn(t.q, d)))

    rd_m().start()
    s_b.mated()
    s_b.stage1()
    rd_m().wait_recv()
    rd_p[...] = rd_own[...] + rd_mate[...]

    @pl.loop(1, n)
    def _(d):
        rd_along_p(d).start()

    s_b.stage1b()
    sum_a = s_a.last()
    s_b.stage2()
    rd_sum = rd_p[...]
    for d in range(1, n):
        rd_along_p(d).wait_recv()
        rd_sum = rd_sum + rd_pin[d]
    rd_q[...] = rd_sum

    @pl.loop(1, n)
    def _(d):
        rd_along_q(d).start()

    own = lax.broadcasted_iota(jnp.int32, (cols, model), 1) == (
        lax.broadcasted_iota(jnp.int32, (cols, model), 0) + t.me * cols
    )
    gain_own = jnp.sum(jnp.where(own, rgain_ref[...], 0.0), axis=1, keepdims=True)
    sum_b = s_b.last()
    grad_a = s_a.collect(sum_a)
    rd_all = rd_q[...]
    for d in range(1, n):
        rd_along_q(d).wait_recv()
        rd_all = rd_all + rd_qin[d]
    grad_b = s_b.collect(sum_b)

    def update(grad, tokens, inv, dots):
        unit = tokens.astype(F32) * inv
        return inv * (gain_own * grad - unit * (dots / model))

    upd_a = update(grad_a, ta_all[t.me], inv_a, rd_all[0:1])
    upd_b = update(grad_b, tb_all[t.me], inv_b, rd_all[1:2])
    grad_img = og_all[t.me, :, LANES : 2 * LANES].astype(F32) + upd_b
    proj_grad = jnp.where(lane < LIVE, grad_img, 0.0).astype(BF16)

    pgrad_ref[...] = proj_grad

    upd = jnp.concatenate([upd_a, upd_b], axis=1)
    high = upd.astype(BF16)
    rest = upd - high.astype(F32)
    mid = rest.astype(BF16)
    small = (rest - mid.astype(F32)).astype(BF16)
    moved = dot(high, perm, NT) + (dot(mid, perm, NT) + dot(small, perm, NT))
    igrad_ref[...] = og_ref[...].astype(F32) + moved

    keep.wait()
    for g in gathers:
        g.drain()
    s_a.drain(act_all)
    s_b.drain(act_all)
    rd_m().wait_send()
    for k in (1, 2):
        most = rd_pin.at[pl.ds(1, n - 1)]
        rd_copy(most, most, k, rd_recv_m.at[0], t.partner).wait_send()


def second_grad_body(pgrad_ref, act_ref, igrad_in, sgrad_ref, igrad_out):
    sgrad_ref[...] = dot(pgrad_ref[...], act_ref[...], NT)

    @pl.when(pl.program_id(0) == 0)
    def _():
        igrad_out[...] = igrad_in[...]


def on_device(
    image_features,
    image_counts,
    slot_position,
    text_ids,
    norm_gain,
    norm_bias,
    proj_first,
    proj_second,
    embedding,
    rms_gain,
    gate_weight,
    up_weight,
    down_weight,
    output_grad,
):
    n = lax.axis_size("tensor_0")
    blocks = 2 * n * n
    seq, cols = output_grad.shape
    model = blocks * cols
    half = n // 2
    vmem = pl.BlockSpec(memory_space=pltpu.VMEM)
    smem = pl.BlockSpec(memory_space=pltpu.SMEM)
    hbm = pl.BlockSpec(memory_space=pl.ANY)
    dma = pltpu.SemaphoreType.DMA
    tile = (cols, LANES)
    hidden = gate_weight.shape[1]
    igrad, pgrad, act = pl.pallas_call(
        kernel_body,
        out_shape=(
            jax.ShapeDtypeStruct((cols, seq), F32),
            jax.ShapeDtypeStruct((cols, LANES), BF16),
            jax.ShapeDtypeStruct((blocks, *tile), BF16),
        ),
        in_specs=[
            vmem,
            smem,
            vmem,
            smem,
            vmem,
            vmem,
            hbm,
            hbm,
            hbm,
            vmem,
            hbm,
            hbm,
            hbm,
            vmem,
        ],
        out_specs=(vmem, vmem, hbm),
        scratch_shapes=[
            pltpu.VMEM(proj_first.shape, BF16),
            pltpu.VMEM(proj_second.shape, BF16),
            pltpu.VMEM((embedding.shape[1] // LANES, cols, LANES), BF16),
            pltpu.VMEM((model, 2 * hidden), BF16),
            pltpu.VMEM(down_weight.shape, BF16),
            pltpu.VMEM((2 * hidden, model), BF16),
            pltpu.VMEM((cols, blocks * LANES), BF16),
            pltpu.VMEM((2, blocks, LANES), F32),
            pltpu.VMEM((blocks, LIVE, LANES), BF16),
            pltpu.VMEM((blocks, *tile), BF16),
            pltpu.VMEM((blocks, cols, seq), BF16),
            pltpu.VMEM((blocks, *tile), BF16),
            pltpu.VMEM((blocks, *tile), BF16),
            pltpu.VMEM((cols, seq), BF16),
            pltpu.VMEM((2, blocks // 2, *tile), F32),
            pltpu.VMEM((2, blocks // 2, *tile), BF16),
            pltpu.VMEM((2, blocks // 2, *tile), BF16),
            pltpu.VMEM((2, half, n, *tile), BF16),
            pltpu.VMEM((2, half, n, *tile), BF16),
            pltpu.VMEM((2, half, n, *tile), BF16),
            pltpu.VMEM((2, half, n, *tile), BF16),
            pltpu.VMEM((2, n, *tile), BF16),
            pltpu.VMEM((2, n, *tile), BF16),
            pltpu.VMEM((8, LANES), F32),
            pltpu.VMEM((8, LANES), F32),
            pltpu.VMEM((8, LANES), F32),
            pltpu.VMEM((n, 8, LANES), F32),
            pltpu.VMEM((8, LANES), F32),
            pltpu.VMEM((n, 8, LANES), F32),
            dma((7,)),
            dma((5, half)),
            dma((5, n - 1, half)),
            dma((5, 1)),
            dma((5,)),
            dma((2, 1)),
            dma((2, 1)),
            dma((3,)),
            dma((n,)),
            dma((n,)),
            dma((1,)),
        ],
        compiler_params=pltpu.CompilerParams(
            collective_id=0, has_side_effects=True, vmem_limit_bytes=64 * 1024 * 1024 - 65536
        ),
        name="projector_step",
    )(
        image_features.T,
        image_counts,
        slot_position.reshape(1, -1),
        text_ids,
        norm_gain.reshape(-1, LANES),
        norm_bias.reshape(-1, LANES),
        proj_first,
        proj_second,
        embedding,
        rms_gain.reshape(1, -1),
        gate_weight,
        up_weight,
        down_weight,
        output_grad.T,
    )
    parts = 2
    sgrad, igrad = pl.pallas_call(
        second_grad_body,
        grid=(parts,),
        out_shape=(
            jax.ShapeDtypeStruct((cols, model), F32),
            jax.ShapeDtypeStruct((cols, seq), F32),
        ),
        in_specs=[
            pl.BlockSpec(tile, lambda k: (0, 0)),
            pl.BlockSpec((model // parts, LANES), lambda k: (k, 0)),
            pl.BlockSpec((cols, seq), lambda k: (0, 0)),
        ],
        out_specs=(
            pl.BlockSpec((cols, model // parts), lambda k: (0, k)),
            pl.BlockSpec((cols, seq), lambda k: (0, 0)),
        ),
        name="second_grad",
    )(pgrad, act.reshape(model, LANES), igrad)
    return igrad.T, sgrad


def solution(mesh):
    torus = Mesh(
        mesh.devices.reshape(mesh.shape["groups"], 8, 8, 2),
        ("groups", "tensor_0", "tensor_1", "tensor_2"),
    )
    in_specs = (
        P("groups", TENSOR),
        P("groups"),
        P("groups"),
        P("groups"),
        P(),
        P(),
        P(TENSOR, None),
        P(TENSOR, None),
        P(TENSOR, None),
        P(),
        P(None, TENSOR),
        P(None, TENSOR),
        P(TENSOR, None),
        P("groups", TENSOR),
    )
    out_specs = (P("groups", TENSOR), P(GROUPS_TENSOR, None))
    return jax.shard_map(
        on_device, mesh=torus, in_specs=in_specs, out_specs=out_specs, check_vma=False
    )
```

```python
import jax
import jax.numpy as jnp
from jax import lax
from jax.experimental import pallas as pl
from jax.experimental.pallas import tpu as pltpu
from jax.sharding import Mesh
from jax.sharding import PartitionSpec as P

LIVE = 80
TENSOR = ("tensor_0", "tensor_1", "tensor_2")
GROUPS_TENSOR = ("groups", "tensor_0", "tensor_1", "tensor_2")
MESH = pl.DeviceIdType.MESH
F32 = jnp.float32
BF16 = jnp.bfloat16
NT = (((1,), (1,)), ((), ()))
NN = (((1,), (0,)), ((), ()))
LANES = 128


def dot(a, b, dims=NN):
    return lax.dot_general(a, b, dims, preferred_element_type=F32)


def erf(x):
    x = jnp.clip(x, -3.832506856900711, 3.832506856900711)
    s = x * x
    top = jnp.full_like(x, 0.00022905065861350646)
    for k in (
        0.0034082910107109506,
        0.050955695062380861,
        0.18520832239976145,
        1.128379143519084,
    ):
        top = top * s + k
    low = jnp.full_like(x, -1.1791602954361697e-7)
    for k in (
        0.000023547966471313185,
        0.0010179625278914885,
        0.014070470171167667,
        0.11098505178285362,
        0.49746925110067538,
        1.0,
    ):
        low = low * s + k
    return x * top / low


class Torus:
    def __init__(self):
        self.c = lax.axis_index("tensor_2")
        self.x = lax.axis_index("tensor_0")
        self.y = lax.axis_index("tensor_1")
        self.n = lax.axis_size("tensor_0")
        self.p = self.pick(self.x, self.y)
        self.q = self.pick(self.y, self.x)
        self.me = self.block(self.p, self.q)
        self.partner = {"tensor_0": self.x, "tensor_1": self.y, "tensor_2": 1 - self.c}

    def pick(self, a, b):
        return (1 - self.c) * a + self.c * b

    def dev(self, p, q):
        return {"tensor_0": self.pick(p, q), "tensor_1": self.pick(q, p), "tensor_2": self.c}

    def chip(self, p, q):
        return self.pick(p, q) * self.n + self.pick(q, p)

    def block(self, p, q):
        return self.chip(p, q) * 2 + self.c

    def row(self, hop, down):
        last = self.n // 2 - 1
        return 2 * last if hop == last else hop + down * last

    def turn(self, a, d):
        return lax.rem(a + d + self.n, self.n)


class Gather:
    def __init__(self, t, buf, near, ring, mate, sent):
        self.t, self.buf = t, buf
        self.near, self.sems, self.mate, self.sent = near, ring, mate, sent

    def copy(self, j, dev, sem):
        return pltpu.make_async_remote_copy(
            self.buf.at[j], self.buf.at[j], self.sent, sem, device_id=dev, device_id_type=MESH
        )

    def to_mate(self, j):
        self.copy(j, self.t.partner, self.mate.at[0]).start()

    def got(self, j, sem):
        self.copy(j, self.t.partner, sem).wait_recv()

    def start(self):
        t = self.t

        @pl.loop(1, t.n)
        def _(d):
            self.copy(t.me, t.dev(t.turn(t.p, d), t.q), self.near.at[lax.div(d, 2)]).start()

        self.to_mate(t.me)

    def up(self, j, k, hop):
        t = self.t
        self.copy(j, t.dev(t.p, t.turn(t.q, 1)), self.sems.at[t.row(hop, 0), k]).start()

    def down(self, j, k, hop):
        t = self.t
        self.copy(j, t.dev(t.p, t.turn(t.q, -1)), self.sems.at[t.row(hop, 1), k]).start()

    def hop0(self):
        t = self.t

        def own(j, k):
            self.up(j, k, 0)
            self.down(j, k, 0)

        own(t.me, 0)
        j = t.block(t.turn(t.p, -1), t.q)
        self.got(j, self.near.at[0])
        own(j, 0)
        self.to_mate(j)

        @pl.loop(1, t.n // 2)
        def _(k):
            self.got(pl.ds(0, 2), self.near.at[k])
            for e in range(2):
                j = t.block(t.turn(t.p, -2 * k - e), t.q)
                own(j, k)
                self.to_mate(j)

    def hop(self, h):
        t = self.t
        half = t.n // 2
        few = half // 2

        def up(k, on):
            self.got(pl.ds(0, 2), self.sems.at[t.row(h - 1, 0), k])
            for e in range(2):
                j = t.block(t.turn(t.p, -2 * k - e), t.turn(t.q, -h))
                if on:
                    self.up(j, k, h)
                self.to_mate(j)

        def down(k, on):
            self.got(pl.ds(0, 2), self.sems.at[t.row(h - 1, 1), k])
            for e in range(2):
                j = t.block(t.turn(t.p, -2 * k - e), t.turn(t.q, h))
                if on:
                    self.down(j, k, h)
                self.to_mate(j)

        if h < half - 1:

            @pl.loop(0, half)
            def _(k):
                up(k, True)
                down(k, True)

        elif h == half - 1:

            @pl.loop(0, few)
            def _(k):
                up(k, True)
                down(k + few, True)
                down(k, False)
                up(k + few, False)

        else:

            @pl.loop(0, few)
            def _(k):
                up(k, False)
                down(k + few, False)

    def finish(self):
        half = self.buf.at[pl.ds(0, self.buf.shape[0] // 2)]
        pltpu.make_async_remote_copy(
            half, half, self.sent, self.mate.at[0], device_id=self.t.partner, device_id_type=MESH
        ).wait_recv()

    def drain(self):
        most = self.buf.at[pl.ds(0, self.buf.shape[0] - 1)]
        pltpu.make_async_remote_copy(
            most, most, self.sent, self.mate.at[0], device_id=self.t.partner, device_id_type=MESH
        ).wait_send()


class Leap(Gather):
    def send(self, j, k, far, dist, down):
        t = self.t
        by = -far if down else far
        sem = self.sems.at[t.row(dist - 1, down), k]
        self.copy(j, t.dev(t.p, t.turn(t.q, by)), sem).start()

    def hop0(self):
        t = self.t

        def own(j, k):
            for far in (2, 1):
                for down in (0, 1):
                    self.send(j, k, far, far, down)

        own(t.me, 0)
        j = t.block(t.turn(t.p, -1), t.q)
        self.got(j, self.near.at[0])
        own(j, 0)
        self.to_mate(j)

        @pl.loop(1, t.n // 2)
        def _(k):
            self.got(pl.ds(0, 2), self.near.at[k])
            for e in range(2):
                j = t.block(t.turn(t.p, -2 * k - e), t.q)
                own(j, k)
                self.to_mate(j)

    def arrived(self, k, dist, down, onward):
        t = self.t
        self.got(pl.ds(0, 2), self.sems.at[t.row(dist - 1, down), k])
        for e in range(2):
            by = dist if down else -dist
            j = t.block(t.turn(t.p, -2 * k - e), t.turn(t.q, by))
            for far in onward:
                self.send(j, k, far, dist + far, down)
            self.to_mate(j)

    def relay(self):
        few = self.t.n // 4

        @pl.loop(0, few)
        def _(k):
            self.arrived(k, 2, 0, (2, 1))
            self.arrived(k + few, 2, 1, (2, 1))

        @pl.loop(0, few)
        def _(k):
            self.arrived(k + few, 2, 0, (1,))
            self.arrived(k, 2, 1, (1,))

    def tail(self, dist):
        @pl.loop(0, self.t.n // 2)
        def _(k):
            self.arrived(k, dist, 0, ())
            self.arrived(k, dist, 1, ())

    def tail4(self):
        few = self.t.n // 4

        @pl.loop(0, few)
        def _(k):
            self.arrived(k, 4, 0, ())
            self.arrived(k + few, 4, 1, ())


class Scatter:
    def __init__(self, t, part, give, take, out_up, out_dn, in_up, in_dn, fin_out, fin_in, sems):
        self.t, self.part, self.give, self.take = t, part, give, take
        self.out_up, self.out_dn, self.in_up, self.in_dn = out_up, out_dn, in_up, in_dn
        self.fin_out, self.fin_in = fin_out, fin_in
        self.sent, self.mate, self.ring, self.near = sems

    def mate_copy(self, span):
        return pltpu.make_async_remote_copy(
            self.give.at[span],
            self.take.at[span],
            self.sent.at[0],
            self.mate.at[0],
            device_id=self.t.partner,
            device_id_type=MESH,
        )

    def fill(self, k, even, odd):
        span = pl.ds(k * even.shape[0], even.shape[0])
        self.part[span] = jnp.where(self.t.c == 0, even, odd)
        self.give[span] = jnp.where(self.t.c == 0, odd, even).astype(BF16)
        self.mate_copy(span).start()

    def mated(self):
        self.mate_copy(pl.ds(0, self.give.shape[0])).wait_recv()

    def base(self, p, q):
        t = self.t
        i = t.chip(p, q)
        return self.part[i] + self.take[i].astype(F32)

    def ring_copy(self, dist, d, down):
        t = self.t
        hop = dist if dist < 3 else dist - 2
        out, into = (self.out_dn, self.in_dn) if down else (self.out_up, self.in_up)
        return pltpu.make_async_remote_copy(
            out.at[dist - 1, d],
            into.at[dist - 1, d],
            self.sent.at[0],
            self.ring.at[t.row(dist - 1, down), lax.div(d, 2)],
            device_id=t.dev(t.p, t.turn(t.q, -hop if down else hop)),
            device_id_type=MESH,
        )

    def pair(self, dist, k, down):
        two = (self.in_dn if down else self.in_up).at[dist - 1, pl.ds(2 * k, 2)]
        pltpu.make_async_remote_copy(
            two,
            two,
            self.sent.at[0],
            self.ring.at[self.t.row(dist - 1, down), k],
            device_id=self.t.partner,
            device_id_type=MESH,
        ).wait_recv()

    def send(self, dist, k, down, had):
        t = self.t
        into = self.in_dn if down else self.in_up
        out = self.out_dn if down else self.out_up
        for h in had:
            self.pair(h, k, down)
        for e in range(2):
            d = 2 * k + e
            value = self.base(t.turn(t.p, -d), t.turn(t.q, -dist if down else dist))
            for h in had:
                value = value + into[h - 1, d].astype(F32)
            out[dist - 1, d] = value.astype(BF16)
            self.ring_copy(dist, d, down).start()

    def stage1(self):
        few = self.t.n // 4

        @pl.loop(0, few)
        def _(k):
            self.send(4, k, 0, ())
            self.send(4, k + few, 1, ())

        @pl.loop(0, 2 * few)
        def _(k):
            self.send(3, k, 0, ())
            self.send(3, k, 1, ())

    def stage1b(self):
        @pl.loop(0, self.t.n // 2)
        def _(k):
            self.send(1, k, 0, ())
            self.send(1, k, 1, ())

    def stage2(self):
        few = self.t.n // 4

        @pl.loop(0, few)
        def _(k):
            self.send(2, k, 0, (3, 4))
            self.send(2, k + few, 1, (3, 4))
            self.send(2, k + few, 0, (3,))
            self.send(2, k, 1, (3,))

    def fin_copy(self, d):
        t = self.t
        return pltpu.make_async_remote_copy(
            self.fin_out.at[d],
            self.fin_in.at[d],
            self.sent.at[0],
            self.near.at[lax.div(d, 2)],
            device_id=t.dev(t.turn(t.p, -d), t.q),
            device_id_type=MESH,
        )

    def whole(self, d):
        value = self.base(self.t.turn(self.t.p, -d), self.t.q)
        for into in (self.in_up, self.in_dn):
            for dist in (1, 2):
                value = value + into[dist - 1, d].astype(F32)
        return value

    def last(self):
        t = self.t

        def both(k):
            for down in (0, 1):
                for dist in (1, 2):
                    self.pair(dist, k, down)

        def give(d):
            self.fin_out[d] = self.whole(d).astype(BF16)
            self.fin_copy(d).start()

        both(0)
        give(1)

        @pl.loop(1, t.n // 2)
        def _(k):
            both(k)
            give(2 * k)
            give(2 * k + 1)

        return self.whole(0)

    def collect(self, value):
        self.fin_copy(1).wait_recv()
        value = value + self.fin_in[1].astype(F32)
        for k in range(1, self.t.n // 2):
            two = self.fin_in.at[pl.ds(2 * k, 2)]
            pltpu.make_async_remote_copy(
                two,
                two,
                self.sent.at[0],
                self.near.at[k],
                device_id=self.t.partner,
                device_id_type=MESH,
            ).wait_recv()
            value = value + self.fin_in[2 * k].astype(F32) + self.fin_in[2 * k + 1].astype(F32)
        return value

    def drain(self, like):
        most = like.at[pl.ds(0, like.shape[0] - 1)]
        pltpu.make_async_remote_copy(
            most, most, self.sent.at[0], self.mate.at[0], device_id=self.t.partner, device_id_type=MESH
        ).wait_send()


def kernel_body(
    feats_hbm,
    counts_hbm,
    pos_hbm,
    ids_hbm,
    ngain_hbm,
    nbias_hbm,
    first_hbm,
    second_hbm,
    emb_hbm,
    rgain_hbm,
    gate_hbm,
    up_hbm,
    down_hbm,
    og_hbm,
    igrad_ref,
    pgrad_ref,
    act_hbm,
    feats_ref,
    counts_ref,
    pos_ref,
    ids_ref,
    ngain_ref,
    nbias_ref,
    rgain_ref,
    og_ref,
    first_v,
    second_v,
    emb_v,
    wcat,
    down_v,
    wt,
    wpad,
    gb_ref,
    feats_all,
    act_all,
    og_all,
    ta_all,
    tb_all,
    text_own,
    part,
    give,
    take,
    out_up,
    out_dn,
    in_up,
    in_dn,
    fin_out,
    fin_in,
    rd_own,
    rd_mate,
    rd_p,
    rd_pin,
    rd_q,
    rd_qin,
    load_sem,
    small_sem,
    near_sem,
    ring_sem,
    mate_sem,
    sent_sem,
    rs_sent,
    rs_mate,
    rd_sent,
    rd_recv_p,
    rd_recv_q,
    rd_recv_m,
):
    t = Torus()
    n = t.n
    blocks = 2 * n * n
    cols, seq = og_ref.shape
    width, slots = feats_ref.shape
    model = blocks * cols
    pix = blocks * width

    barrier = pltpu.get_barrier_semaphore()

    @pl.loop(1, n)
    def _(d):
        pl.semaphore_signal(
            barrier, inc=1, device_id=t.dev(t.turn(t.p, d), t.q), device_id_type=MESH
        )
        pl.semaphore_signal(
            barrier, inc=1, device_id=t.dev(t.p, t.turn(t.q, d)), device_id_type=MESH
        )

    pl.semaphore_signal(barrier, inc=1, device_id=t.partner, device_id_type=MESH)

    loads = [
        pltpu.make_async_copy(first_hbm, first_v, load_sem.at[0]),
        pltpu.make_async_copy(gate_hbm, wcat.at[:, pl.ds(0, LANES)], load_sem.at[1]),
        pltpu.make_async_copy(up_hbm, wcat.at[:, pl.ds(LANES, LANES)], load_sem.at[2]),
        pltpu.make_async_copy(second_hbm, second_v, load_sem.at[3]),
        pltpu.make_async_copy(down_hbm, down_v, load_sem.at[4]),
    ]
    smalls = [
        pltpu.make_async_copy(src, dst, small_sem.at[k])
        for k, (src, dst) in enumerate(
            (
                (feats_hbm, feats_ref),
                (counts_hbm, counts_ref),
                (pos_hbm, pos_ref),
                (ids_hbm, ids_ref),
                (ngain_hbm, ngain_ref),
                (nbias_hbm, nbias_ref),
                (rgain_hbm, rgain_ref),
                (og_hbm, og_ref),
            )
        )
    ]
    for small in smalls:
        small.start()
    loads[0].start()
    smalls[0].wait()
    smalls[1].wait()

    slot = lax.broadcasted_iota(jnp.int32, (LIVE, slots), 1)
    row = lax.broadcasted_iota(jnp.int32, (LIVE, slots), 0)
    images = counts_ref.shape[0]
    per = slots // images
    at = slot % per
    live = jnp.zeros((LIVE, slots), jnp.int32)
    rank = at
    before = 0
    for k in range(images):
        count = counts_ref[k]
        here = (slot // per) == k
        live = jnp.where(here & (at < count), 1, live)
        rank = jnp.where(here, at + before, rank)
        before = before + count
    choose = jnp.where((live == 1) & (rank == row), 1.0, 0.0).astype(BF16)
    feats_own = dot(choose, feats_ref[...], NT)
    feats_all[t.me] = jnp.zeros((LIVE, LANES), BF16)
    feats_all[t.me, :, 0:width] = feats_own.astype(BF16)

    gathers = []
    for k, buf in enumerate((feats_all, og_all, ta_all, act_all, tb_all)):
        kind = Gather if k in (1, 2) else Leap
        gathers.append(
            kind(t, buf, near_sem.at[k], ring_sem.at[k], mate_sem.at[k], sent_sem.at[k])
        )
    g_feats, g_og, g_ta, g_act, g_tb = gathers

    pl.semaphore_wait(barrier, 2 * (n - 1) + 1)
    g_feats.start()

    @pl.loop(0, emb_v.shape[0], unroll=8)
    def _(k):
        span = pl.ds(pl.multiple_of(k * LANES, LANES), LANES)
        pltpu.make_async_copy(emb_hbm.at[:, span], emb_v.at[k], load_sem.at[5]).start()

    for load in loads[1:]:
        load.start()

    smalls[2].wait()
    smalls[7].wait()
    pos = pos_ref[...]
    where_row = lax.broadcasted_iota(jnp.int32, (seq, slots), 0)
    hit = jnp.where((where_row == pos) & (live[0:1] == 1), 1.0, 0.0)
    is_img = jnp.sum(hit, axis=1, keepdims=True)
    img_rank = jnp.sum(hit * rank[0:1].astype(F32), axis=1, keepdims=True)
    low = jnp.where(
        lax.broadcasted_iota(jnp.int32, (seq, seq), 1)
        < lax.broadcasted_iota(jnp.int32, (seq, seq), 0),
        1.0,
        0.0,
    ).astype(BF16)
    not_img = jnp.broadcast_to(1.0 - is_img, (seq, LANES)).astype(BF16)
    text_rank = dot(low, not_img)[:, 0:1]
    text_col = jnp.where(text_rank < LANES, text_rank, text_rank + LIVE)
    col_of = jnp.where(is_img > 0.5, LANES + img_rank, text_col)
    perm = jnp.where(
        lax.broadcasted_iota(jnp.int32, (seq, seq), 1).astype(F32) == col_of, 1.0, 0.0
    ).astype(BF16)
    og_packed = dot(og_ref[...], perm).astype(BF16)
    og_all[t.me] = og_packed
    g_og.start()

    loads[0].wait()
    smalls[4].wait()
    smalls[5].wait()
    wpad[...] = jnp.zeros(wpad.shape, BF16)
    gb_ref[...] = jnp.zeros(gb_ref.shape, F32)
    for j in range(blocks):
        wpad[:, LANES * j : LANES * j + width] = first_v[:, width * j : width * (j + 1)]
        line, start = divmod(width * j, LANES)
        fit = min(width, LANES - start)
        for k, ref in enumerate((ngain_ref, nbias_ref)):
            gb_ref[k, j : j + 1, 0:fit] = ref[line : line + 1, start : start + fit]
            if fit < width:
                gb_ref[k, j : j + 1, fit:width] = ref[line + 1 : line + 2, 0 : width - fit]

    pltpu.make_async_copy(emb_v, emb_v, load_sem.at[5]).wait()
    smalls[3].wait()
    lane = lax.broadcasted_iota(jnp.int32, (cols, LANES), 1)

    def embed(tile):
        def one(k, acc):
            word = ids_ref[tile * LANES + k]
            inside = lax.rem(word, LANES)
            found = emb_v[lax.div(word, LANES)].astype(F32)
            column = jnp.sum(jnp.where(lane == inside, found, 0.0), axis=1, keepdims=True)
            return jnp.where(lane == k, column, acc)

        text_own[:, pl.ds(tile * LANES, LANES)] = lax.fori_loop(
            0, LANES, one, jnp.zeros((cols, LANES), F32), unroll=8
        ).astype(BF16)

    embed(0)

    shift = feats_all[t.me].astype(F32)[:, 0:1]
    band = 16
    bands = LIVE // band

    def sums_of(count, block_at, carry):
        out = []
        for r in range(bands):
            rows = pl.ds(r * band, band)
            about = jnp.broadcast_to(shift[r * band : (r + 1) * band], (band, LANES))

            def add_up(k, pair):
                moved = feats_all[block_at(k), rows].astype(F32) - about
                return pair[0] + moved, pair[1] + moved * moved

            out.append(lax.fori_loop(0, count, add_up, carry[r], unroll=8))
        return out

    def line(off):
        return lambda k: t.block(k, t.turn(t.q, off))

    zero = jnp.zeros((band, LANES), F32)
    sums = [(zero, zero)] * bands
    g_feats.hop0()
    sums = sums_of(n, line(0), sums)
    embed(1)
    text_packed = dot(text_own[...], perm)
    text_a = text_packed[:, 0:LANES]
    text_b_tile = text_packed[:, LANES : 2 * LANES]
    ta_all[t.me] = text_a.astype(BF16)
    g_ta.start()
    g_feats.relay()
    g_og.hop0()
    for off in (2, -2):
        sums = sums_of(n, line(off), sums)
    g_feats.tail(1)
    for off in (1, -1):
        sums = sums_of(n, line(off), sums)
    g_feats.tail(3)
    for off in (3, -3):
        sums = sums_of(n, line(off), sums)
    g_feats.tail4()
    sums = sums_of(n, line(n // 2), sums)
    g_feats.finish()
    sums = sums_of(blocks // 2, lambda k: 2 * k + 1 - t.c, sums)
    sums = [jnp.concatenate([sums[r][e] for r in range(bands)], axis=0) for e in range(2)]
    inside = lax.broadcasted_iota(jnp.int32, (LIVE, LANES), 1) < width
    off = jnp.sum(jnp.where(inside, sums[0], 0.0), axis=1, keepdims=True) / pix
    square = jnp.sum(jnp.where(inside, sums[1], 0.0), axis=1, keepdims=True) / pix
    mean = shift + off
    scale = lax.rsqrt(jnp.maximum(square - off * off, 0.0) + 1e-05)
    g_og.hop(1)
    g_ta.hop0()

    fold = 8

    def first_step(k, acc):
        tiles = []
        for e in range(fold):
            j = k * fold + e
            centre = feats_all[j].astype(F32) - mean
            value = centre * scale * gb_ref[0, pl.ds(j, 1), :] + gb_ref[1, pl.ds(j, 1), :]
            tiles.append(value.astype(BF16))
        span = pl.ds(pl.multiple_of(k * fold * LANES, fold * LANES), fold * LANES)
        return acc + dot(wpad[:, span], jnp.concatenate(tiles, axis=1), NT)

    hidden = lax.fori_loop(
        0, blocks // fold, first_step, jnp.zeros((cols, LIVE), F32), unroll=4
    )
    hidden = 0.5 * hidden * (1.0 + erf(hidden * 0.7071067811865476))
    act_all[t.me] = jnp.zeros((cols, LANES), BF16)
    act_all[t.me, :, 0:LIVE] = hidden.astype(BF16)
    g_act.start()

    loads[1].wait()
    loads[2].wait()
    smalls[6].wait()
    big_eye = jnp.where(
        lax.broadcasted_iota(jnp.int32, (seq, seq), 1)
        == lax.broadcasted_iota(jnp.int32, (seq, seq), 0),
        1.0,
        0.0,
    ).astype(BF16)

    def turn_weights(a, b):
        @pl.loop(a, b, unroll=2)
        def _(k):
            at_row = pl.multiple_of(k * seq, seq)
            flipped = dot(big_eye, wcat[pl.ds(at_row, seq), :], NT)
            wt[:, pl.ds(at_row, seq)] = (flipped * rgain_ref[:, pl.ds(at_row, seq)]).astype(BF16)

    pieces = model // seq
    cut = [pieces * k // 6 for k in range(7)]
    g_og.hop(2)
    turn_weights(cut[0], cut[1])
    g_ta.hop(1)
    turn_weights(cut[1], cut[2])
    g_act.hop0()
    g_og.hop(3)
    turn_weights(cut[2], cut[3])
    g_ta.hop(2)
    turn_weights(cut[3], cut[4])
    g_act.relay()
    g_act.tail(1)
    g_ta.hop(3)
    turn_weights(cut[4], cut[5])
    g_og.hop(4)
    turn_weights(cut[5], cut[6])
    g_act.tail(3)
    g_act.tail4()
    g_act.finish()
    keep = pltpu.make_async_copy(act_all, act_hbm, load_sem.at[6])
    keep.start()

    loads[3].wait()
    group = blocks // 8
    span_rows = group * cols

    def rows_of(buf, k):
        return buf[pl.ds(k * group, group)].reshape(span_rows, buf.shape[2])

    def second_step(k, acc):
        span = pl.ds(pl.multiple_of(k * span_rows, span_rows), span_rows)
        return acc + dot(second_v[:, span], rows_of(act_all, k))

    projected = lax.fori_loop(0, 8, second_step, jnp.zeros((cols, LANES), F32), unroll=8)
    tb_all[t.me] = jnp.where(lane < LIVE, projected, text_b_tile).astype(BF16)
    g_tb.start()

    g_ta.hop(4)
    g_og.finish()
    loads[4].wait()

    def down_step(k, acc):
        span = pl.ds(pl.multiple_of(k * span_rows, span_rows), span_rows)
        return acc + dot(down_v[:, span], rows_of(og_all, k))

    hidden_grad = lax.fori_loop(0, 8, down_step, jnp.zeros((LANES, seq), F32), unroll=4)
    scatters = []
    for k, share in enumerate((0, 3)):
        scatters.append(
            Scatter(
                t,
                part.at[k],
                give.at[k],
                take.at[k],
                out_up.at[k],
                out_dn.at[k],
                in_up.at[k],
                in_dn.at[k],
                fin_out.at[k],
                fin_in.at[k],
                (rs_sent.at[k], rs_mate.at[k], ring_sem.at[share], near_sem.at[share]),
            )
        )
    s_a, s_b = scatters

    def gates(buf, hid):
        def step(k, carry):
            acc, sq = carry
            rows = rows_of(buf, k)
            span = pl.ds(pl.multiple_of(k * span_rows, span_rows), span_rows)
            wide = rows.astype(F32)
            sq = sq + jnp.sum(wide * wide, axis=0, keepdims=True)
            return acc + dot(wt[:, span], rows), sq

        acc, sq = lax.fori_loop(
            0,
            8,
            step,
            (jnp.zeros((2 * LANES, LANES), F32), jnp.zeros((1, LANES), F32)),
            unroll=4,
        )
        inv = lax.rsqrt(sq / model + 1e-05)
        acc = acc * inv
        gate, up = acc[0:LANES], acc[LANES : 2 * LANES]
        sig = 1.0 / (1.0 + jnp.exp(-gate))
        gate_grad = (hid * up * sig * (1.0 + gate * (1.0 - sig))).astype(BF16)
        up_grad = (hid * gate * sig).astype(BF16)
        dots = jnp.sum(
            gate_grad.astype(F32) * gate + up_grad.astype(F32) * up, axis=0, keepdims=True
        )
        both = jnp.concatenate([gate_grad, up_grad], axis=0)

        return inv, dots, both

    def spread_out(both, scatter):
        some = 2 * group
        part_rows = some * cols

        @pl.loop(0, blocks // some)
        def _(k):
            at_row = pl.multiple_of(k * part_rows, part_rows)
            value = dot(wcat[pl.ds(at_row, part_rows), :], both)
            value = value.reshape(some // 2, 2, cols, LANES)
            scatter.fill(k, value[:, 0], value[:, 1])

    g_ta.finish()
    inv_a, dots_a, both_a = gates(ta_all, hidden_grad[:, 0:LANES])
    g_tb.hop0()
    spread_out(both_a, s_a)
    g_tb.relay()
    s_a.mated()
    s_a.stage1()
    g_tb.tail(1)
    s_a.stage1b()
    g_tb.tail(3)
    g_tb.tail4()
    g_tb.finish()
    inv_b, dots_b, both_b = gates(tb_all, hidden_grad[:, LANES : 2 * LANES])
    s_a.stage2()
    spread_out(both_b, s_b)

    rd_own[...] = jnp.zeros(rd_own.shape, F32)
    rd_own[0:1] = dots_a
    rd_own[1:2] = dots_b

    def rd_copy(src, dst, sem_at, recv, dev):
        return pltpu.make_async_remote_copy(
            src, dst, rd_sent.at[sem_at], recv, device_id=dev, device_id_type=MESH
        )

    def rd_m():
        return rd_copy(rd_own, rd_mate, 0, rd_recv_m.at[0], t.partner)

    def rd_along_p(d):
        return rd_copy(rd_p, rd_pin.at[d], 1, rd_recv_p.at[d], t.dev(t.turn(t.p, d), t.q))

    def rd_along_q(d):
        return rd_copy(rd_q, rd_qin.at[d], 2, rd_recv_q.at[d], t.dev(t.p, t.turn(t.q, d)))

    rd_m().start()
    s_b.mated()
    s_b.stage1()
    rd_m().wait_recv()
    rd_p[...] = rd_own[...] + rd_mate[...]

    @pl.loop(1, n)
    def _(d):
        rd_along_p(d).start()

    s_b.stage1b()
    sum_a = s_a.last()
    s_b.stage2()
    rd_sum = rd_p[...]
    for d in range(1, n):
        rd_along_p(d).wait_recv()
        rd_sum = rd_sum + rd_pin[d]
    rd_q[...] = rd_sum

    @pl.loop(1, n)
    def _(d):
        rd_along_q(d).start()

    own = lax.broadcasted_iota(jnp.int32, (cols, model), 1) == (
        lax.broadcasted_iota(jnp.int32, (cols, model), 0) + t.me * cols
    )
    gain_own = jnp.sum(jnp.where(own, rgain_ref[...], 0.0), axis=1, keepdims=True)
    sum_b = s_b.last()
    grad_a = s_a.collect(sum_a)
    rd_all = rd_q[...]
    for d in range(1, n):
        rd_along_q(d).wait_recv()
        rd_all = rd_all + rd_qin[d]
    grad_b = s_b.collect(sum_b)

    def update(grad, tokens, inv, dots):
        unit = tokens.astype(F32) * inv
        return inv * (gain_own * grad - unit * (dots / model))

    upd_a = update(grad_a, ta_all[t.me], inv_a, rd_all[0:1])
    upd_b = update(grad_b, tb_all[t.me], inv_b, rd_all[1:2])
    grad_img = og_all[t.me, :, LANES : 2 * LANES].astype(F32) + upd_b
    proj_grad = jnp.where(lane < LIVE, grad_img, 0.0).astype(BF16)

    pgrad_ref[...] = proj_grad

    upd = jnp.concatenate([upd_a, upd_b], axis=1)
    high = upd.astype(BF16)
    rest = upd - high.astype(F32)
    mid = rest.astype(BF16)
    small = (rest - mid.astype(F32)).astype(BF16)
    moved = dot(high, perm, NT) + (dot(mid, perm, NT) + dot(small, perm, NT))
    igrad_ref[...] = og_ref[...].astype(F32) + moved

    keep.wait()
    for g in gathers:
        g.drain()
    s_a.drain(act_all)
    s_b.drain(act_all)
    rd_m().wait_send()
    for k in (1, 2):
        most = rd_pin.at[pl.ds(1, n - 1)]
        rd_copy(most, most, k, rd_recv_m.at[0], t.partner).wait_send()


def second_grad_body(pgrad_ref, act_ref, igrad_in, sgrad_ref, igrad_out):
    sgrad_ref[...] = dot(pgrad_ref[...], act_ref[...], NT)

    @pl.when(pl.program_id(0) == 0)
    def _():
        igrad_out[...] = igrad_in[...]


def on_device(
    image_features,
    image_counts,
    slot_position,
    text_ids,
    norm_gain,
    norm_bias,
    proj_first,
    proj_second,
    embedding,
    rms_gain,
    gate_weight,
    up_weight,
    down_weight,
    output_grad,
):
    n = lax.axis_size("tensor_0")
    blocks = 2 * n * n
    seq, cols = output_grad.shape
    model = blocks * cols
    half = n // 2
    vmem = pl.BlockSpec(memory_space=pltpu.VMEM)
    hbm = pl.BlockSpec(memory_space=pl.ANY)
    dma = pltpu.SemaphoreType.DMA
    tile = (cols, LANES)
    hidden = gate_weight.shape[1]
    igrad, pgrad, act = pl.pallas_call(
        kernel_body,
        out_shape=(
            jax.ShapeDtypeStruct((cols, seq), F32),
            jax.ShapeDtypeStruct((cols, LANES), BF16),
            jax.ShapeDtypeStruct((blocks, *tile), BF16),
        ),
        in_specs=[hbm] * 14,
        out_specs=(vmem, vmem, hbm),
        scratch_shapes=[
            pltpu.VMEM(image_features.shape[::-1], BF16),
            pltpu.SMEM(image_counts.shape, jnp.int32),
            pltpu.VMEM((1, slot_position.shape[0]), jnp.int32),
            pltpu.SMEM(text_ids.shape, jnp.int32),
            pltpu.VMEM((norm_gain.shape[0] // LANES, LANES), F32),
            pltpu.VMEM((norm_bias.shape[0] // LANES, LANES), F32),
            pltpu.VMEM((1, model), F32),
            pltpu.VMEM((cols, seq), BF16),
            pltpu.VMEM(proj_first.shape, BF16),
            pltpu.VMEM(proj_second.shape, BF16),
            pltpu.VMEM((embedding.shape[1] // LANES, cols, LANES), BF16),
            pltpu.VMEM((model, 2 * hidden), BF16),
            pltpu.VMEM(down_weight.shape, BF16),
            pltpu.VMEM((2 * hidden, model), BF16),
            pltpu.VMEM((cols, blocks * LANES), BF16),
            pltpu.VMEM((2, blocks, LANES), F32),
            pltpu.VMEM((blocks, LIVE, LANES), BF16),
            pltpu.VMEM((blocks, *tile), BF16),
            pltpu.VMEM((blocks, cols, seq), BF16),
            pltpu.VMEM((blocks, *tile), BF16),
            pltpu.VMEM((blocks, *tile), BF16),
            pltpu.VMEM((cols, seq), BF16),
            pltpu.VMEM((2, blocks // 2, *tile), F32),
            pltpu.VMEM((2, blocks // 2, *tile), BF16),
            pltpu.VMEM((2, blocks // 2, *tile), BF16),
            pltpu.VMEM((2, half, n, *tile), BF16),
            pltpu.VMEM((2, half, n, *tile), BF16),
            pltpu.VMEM((2, half, n, *tile), BF16),
            pltpu.VMEM((2, half, n, *tile), BF16),
            pltpu.VMEM((2, n, *tile), BF16),
            pltpu.VMEM((2, n, *tile), BF16),
            pltpu.VMEM((8, LANES), F32),
            pltpu.VMEM((8, LANES), F32),
            pltpu.VMEM((8, LANES), F32),
            pltpu.VMEM((n, 8, LANES), F32),
            pltpu.VMEM((8, LANES), F32),
            pltpu.VMEM((n, 8, LANES), F32),
            dma((7,)),
            dma((8,)),
            dma((5, half)),
            dma((5, n - 1, half)),
            dma((5, 1)),
            dma((5,)),
            dma((2, 1)),
            dma((2, 1)),
            dma((3,)),
            dma((n,)),
            dma((n,)),
            dma((1,)),
        ],
        compiler_params=pltpu.CompilerParams(
            collective_id=0, has_side_effects=True, vmem_limit_bytes=64 * 1024 * 1024 - 65536
        ),
        name="projector_step",
    )(
        image_features.T,
        image_counts,
        slot_position.reshape(1, -1),
        text_ids,
        norm_gain.reshape(-1, LANES),
        norm_bias.reshape(-1, LANES),
        proj_first,
        proj_second,
        embedding,
        rms_gain.reshape(1, -1),
        gate_weight,
        up_weight,
        down_weight,
        output_grad.T,
    )
    parts = 2
    sgrad, igrad = pl.pallas_call(
        second_grad_body,
        grid=(parts,),
        out_shape=(
            jax.ShapeDtypeStruct((cols, model), F32),
            jax.ShapeDtypeStruct((cols, seq), F32),
        ),
        in_specs=[
            pl.BlockSpec(tile, lambda k: (0, 0)),
            pl.BlockSpec((model // parts, LANES), lambda k: (k, 0)),
            pl.BlockSpec((cols, seq), lambda k: (0, 0)),
        ],
        out_specs=(
            pl.BlockSpec((cols, model // parts), lambda k: (0, k)),
            pl.BlockSpec((cols, seq), lambda k: (0, 0)),
        ),
        name="second_grad",
    )(pgrad, act.reshape(model, LANES), igrad)
    return igrad.T, sgrad


def solution(mesh):
    torus = Mesh(
        mesh.devices.reshape(mesh.shape["groups"], 8, 8, 2),
        ("groups", "tensor_0", "tensor_1", "tensor_2"),
    )
    in_specs = (
        P("groups", TENSOR),
        P("groups"),
        P("groups"),
        P("groups"),
        P(),
        P(),
        P(TENSOR, None),
        P(TENSOR, None),
        P(TENSOR, None),
        P(),
        P(None, TENSOR),
        P(None, TENSOR),
        P(TENSOR, None),
        P("groups", TENSOR),
    )
    out_specs = (P("groups", TENSOR), P(GROUPS_TENSOR, None))
    return jax.shard_map(
        on_device, mesh=torus, in_specs=in_specs, out_specs=out_specs, check_vma=False
    )
```
